32 devices in a mesh: ep: 8 (over z, x), corner: 4 (over y, core).
Axes of the slice: x: 2, y: 2, z: 4, core: 2. Of those that a mesh axis runs over, the one named last changes fastest.
Arguments:
- required: float32 [8, 262144], P('corner', 'ep'), may hold values from -3 to 3
- arrival: float32 [8, 262144], P('corner', 'ep'), may hold values from -7.2 to 7.2
- hold_required: float32 [8, 262144], P('corner', 'ep'), may hold values from -5.4 to 5.4
- early_arrival: float32 [8, 262144], P('corner', 'ep'), may hold values from -3 to 3
- part_ids: int32 [262144], P('ep'), may hold values from 0 to 63
- bin_edges: int32 [512], replicated, may hold values from -4096 to -1, as said below
Outputs:
- part_hist: float32 [64, 8, 2, 512], P(None, 'corner')
- part_tns: float32 [64, 8, 2], P(None, 'corner')
- part_share: float32 [64], replicated
- tns: float32 [8, 2], P('corner')
- wns: float32 [8, 2], P('corner')
- worst: float32 [2, 262144], P(None, 'ep')
The draws below stay inside these ranges and needn't reach their ends.
Inputs may be any that keep to these rules, and one draw needn't show every extreme that they name: `bin_edges`: strictly increasing and negative; consecutive nodes differ by 1 to 8.
All inputs are finite; a program needn't handle non-finite values.
Results may differ from the reference program's by a relative error of at most 0.0003.
Values sent between devices are 32-bit elements; how exact they have to be, the bound alone decides.
A program may use at most 64 MiB of HBM per device.

```python
import math
import jax
import jax.numpy as jnp
import numpy as np
from jax import lax

BINS = 512
GROUPS = 64
CORNERS = 8
ENDPOINTS = 262144


def rising(key, scale):
    position = jnp.arange(ENDPOINTS, dtype=jnp.float32) / ENDPOINTS
    factor = 1.0 + 2.0 * position
    values = scale * factor * jax.random.normal(key, (CORNERS, ENDPOINTS), jnp.float32)
    return jnp.clip(values, -18.0 * scale, 18.0 * scale)


def draw_arrival(key, part):
    return rising(jax.random.fold_in(key, 11), 0.4)


def draw_hold_required(key, part):
    return rising(jax.random.fold_in(key, 23), 0.3)


def draw_bin_edges(key, part):
    gaps = jax.random.randint(jax.random.fold_in(key, 37), (BINS,), 1, 9, jnp.int32)
    return (-jnp.cumsum(gaps)[::-1]).astype(jnp.int32)


def with_ends(result, rng, low, largest):
    spot = [jax.random.randint(jax.random.fold_in(rng, axis), (), 0, length) for axis, length in enumerate(result.shape)]
    longest = result.shape.index(max(result.shape))
    neighbour = spot[:longest] + [(spot[longest] + 1) % result.shape[longest]] + spot[longest + 1:]
    return result.at[tuple(spot)].set(low).at[tuple(neighbour)].set(largest)


def shard_levels(stream_key, dims, shards, least, top_value):
    loudness, own = 1.0, jax.random.fold_in(stream_key, 6)
    for dim, blocks in shards:
        steps = jnp.exp(jax.random.uniform(jax.random.fold_in(own, dim), (blocks,), jnp.float32, least / len(shards), top_value / len(shards)))
        loudness = loudness * jnp.repeat(steps, dims[dim] // blocks).reshape([-1 if axis == dim else 1 for axis in range(len(dims))])
    return loudness


def rank_bounds(amount, lean):
    weights = [(1 << 20) // math.isqrt(rank ** lean) + 1 for rank in range(1, amount + 1)]
    deviation = 1 + sum(weights) // (1 << 30)
    return np.cumsum(np.array([max(1, weight // deviation) for weight in weights]))


def ranked(own_key, dims, count, slope):
    listing = rank_bounds(count, slope)
    ticket = jax.random.randint(jax.random.fold_in(own_key, 1), dims, 0, int(listing[count - 1]))
    rank = jnp.searchsorted(jnp.asarray(listing, jnp.int32), ticket, side="right")
    return jax.random.permutation(jax.random.fold_in(own_key, 2), count)[rank].astype(jnp.int32)


def centred(stream_key, dims, deviation, limit, pieces=(), kind=jnp.bfloat16):
    level = shard_levels(stream_key, dims, pieces, -0.22, 0.18) if pieces else 1.0
    entries = jax.random.normal(stream_key, dims, jnp.float32) * deviation * level
    return jnp.minimum(jnp.maximum(entries, -limit), limit).astype(kind)


def setup_inputs(seed: int = 0) -> dict:
    splits = jax.random.split(jax.random.key(seed), 7)
    required = centred(splits[0], (CORNERS, ENDPOINTS), 0.5, 3.0, ((0, 4), (1, 8)), jnp.float32)
    arrival = draw_arrival(jax.random.fold_in(splits[6], 71), 0)
    hold_required = draw_hold_required(jax.random.fold_in(splits[6], 71), 0)
    early_arrival = centred(splits[3], (CORNERS, ENDPOINTS), 0.5, 3.0, ((0, 4), (1, 8)), jnp.float32)
    part_ids = with_ends(ranked(splits[4], (ENDPOINTS,), GROUPS, 1), jax.random.fold_in(splits[4], 3), 0, GROUPS - 1).astype(jnp.int32)
    bin_edges = draw_bin_edges(jax.random.fold_in(splits[6], 71), 0)
    return dict(required=required, arrival=arrival, hold_required=hold_required, early_arrival=early_arrival, part_ids=part_ids, bin_edges=bin_edges)


def node_tables(bin_edges):
    nodes = bin_edges.astype(jnp.float32) * 0.001
    upper = jnp.concatenate([nodes[1:], jnp.zeros((1,), jnp.float32)])
    lower = jnp.concatenate([nodes[:1] - 1.0, nodes[:-1]])
    return nodes, lower, upper


def weights_at(index, level, nodes, lower, upper):
    node = nodes[index]
    low = lower[index]
    high = upper[index]
    rise = (level - low) / (node - low)
    fall = (high - level) / (high - node)
    return jnp.maximum(jnp.minimum(rise, fall), 0.0)


def rounded(values):
    narrow = lax.optimization_barrier(values.astype(jnp.bfloat16))
    return narrow.astype(jnp.float32)


def histogram(slack, part_ids, nodes, lower, upper):
    level = jnp.clip(slack, nodes[0], 0.0)
    first = jnp.searchsorted(nodes, level, side="right").astype(jnp.int32) - 1
    first = jnp.clip(first, 0, BINS - 1).astype(jnp.int32)
    second = jnp.minimum(first + 1, BINS - 1).astype(jnp.int32)
    w_first = rounded(weights_at(first, level, nodes, lower, upper))
    w_second = rounded(jnp.where(first + 1 < BINS, weights_at(second, level, nodes, lower, upper), 0.0))
    total = jax.ops.segment_sum(w_first, part_ids * BINS + first, num_segments=GROUPS * BINS)
    total = total + jax.ops.segment_sum(w_second, part_ids * BINS + second, num_segments=GROUPS * BINS)
    return total.reshape(GROUPS, BINS)


def reference(required, arrival, hold_required, early_arrival, part_ids, bin_edges):
    nodes, lower, upper = node_tables(bin_edges)
    setup = required - arrival
    hold = early_arrival - hold_required

    def one_corner(pair):
        return jnp.stack([histogram(pair[0], part_ids, nodes, lower, upper), histogram(pair[1], part_ids, nodes, lower, upper)], axis=1)

    hists = lax.map(one_corner, (setup, hold))
    density = GROUPS * BINS / ENDPOINTS
    part_hist = jnp.transpose(hists, (1, 0, 2, 3)) * density
    neg_setup = jnp.minimum(setup, 0.0)
    neg_hold = jnp.minimum(hold, 0.0)
    share = GROUPS / ENDPOINTS
    part_setup = jax.ops.segment_sum(neg_setup.T, part_ids, num_segments=GROUPS)
    part_holdn = jax.ops.segment_sum(neg_hold.T, part_ids, num_segments=GROUPS)
    part_tns = jnp.stack([part_setup, part_holdn], axis=2) * share
    counts = jax.ops.segment_sum(jnp.ones(part_ids.shape, jnp.float32), part_ids, num_segments=GROUPS)
    part_share = counts * share
    tns = jnp.stack([jnp.sum(neg_setup, axis=1), jnp.sum(neg_hold, axis=1)], axis=1) * (1.0 / ENDPOINTS)
    wns = jnp.stack([jnp.min(setup, axis=1), jnp.min(hold, axis=1)], axis=1)
    worst = jnp.stack([jnp.min(setup, axis=0), jnp.min(hold, axis=0)], axis=0)
    return (part_hist, part_tns, part_share, tns, wns, worst)
```

```python
import functools
import jax
import jax.numpy as jnp
from jax import lax
from jax.experimental import pallas as pl
from jax.experimental.pallas import tpu as pltpu
from jax.sharding import PartitionSpec as P

GROUPS = 64
LANES = 128
SUBS = 8
PACK = 16
PAIR = 2
FIELDS = 4
MESH = pl.DeviceIdType.MESH


def pick(table, index):
    return jnp.take_along_axis(table, index, axis=1, mode="promise_in_bounds")


def make_tables(edges_ref):
    nodes = edges_ref[...].astype(jnp.float32) * 0.001
    lane = lax.broadcasted_iota(jnp.int32, (SUBS, LANES), 1)
    rows = [jnp.broadcast_to(nodes[q : q + 1], (SUBS, LANES)) for q in range(4)]

    def gathered(place):
        index = place & (LANES - 1)
        value = pick(rows[3], index)
        for q in (2, 1, 0):
            value = jnp.where(place < LANES * (q + 1), pick(rows[q], index), value)
        return value

    def same(row):
        return pick(row, jnp.zeros((SUBS, LANES), jnp.int32))

    steps = []
    for k in range(2, 8):
        steps.append(gathered(((lane << (9 - k)) + (1 << (8 - k))) & 511))
    last = [gathered(2 * lane + 1), gathered(2 * lane + 2 * LANES + 1)]
    return [same(row) for row in rows], steps, last


def search(tables, slack):
    quarter, steps, last = tables
    level = jnp.minimum(jnp.maximum(slack, quarter[0]), 0.0)
    top = level >= quarter[2]
    low = jnp.where(top, quarter[2], quarter[0])
    high = jnp.where(top, 0.0, quarter[2])
    value = jnp.where(top, quarter[3], quarter[1])
    above = level >= value
    low = jnp.where(above, value, low)
    high = jnp.where(above, high, value)
    index = jnp.where(top, 2, 0) + jnp.where(above, 1, 0)
    part = index
    for table in steps:
        value = pick(table, index)
        above = level >= value
        low = jnp.where(above, value, low)
        high = jnp.where(above, high, value)
        index = index + index
        index = jnp.where(above, index + 1, index)
    place = index & (LANES - 1)
    value = jnp.where(top, pick(last[1], place), pick(last[0], place))
    above = level >= value
    low = jnp.where(above, value, low)
    high = jnp.where(above, high, value)
    scale = 1.0 / (high - low)
    first = (high - level) * scale
    second = (level - low) * scale
    odd_at = index & 63
    even_at = jnp.where(above, odd_at + 1, odd_at)
    even = jnp.where(above, second, first)
    odd = jnp.where(above, first, second)
    return part, even_at, odd_at, even, odd


def report_kernel(
    n, nc, density, plan,
    req, arr, hreq, early, ids, edges,
    hist_out, stats_out, worst_out,
    marks, codes, tail, acc, worst, worst_in, least,
    hist, pair_in, line_in, all_in, stats, stats_in,
    ps, pr, ls, lr, gs, gr, fs, fr, ss, sr, ws, wr, vs, vr,
):
    corners = hist.shape[0] // 2
    combos = 2 * corners
    blocks = ids.shape[0]
    steps = blocks // SUBS
    depth = steps * LANES
    chunk = GROUPS // n
    line = n // PAIR
    share = worst_out.shape[0] // nc
    narrow = jnp.bfloat16
    f32 = jnp.float32
    me = lax.axis_index("ep")
    mc = lax.axis_index("corner")
    mx = lax.rem(me, PAIR)
    mz = me // PAIR
    other = PAIR - 1 - mx
    mine = mx * line + mz

    barrier = pltpu.get_barrier_semaphore()
    for d in range(1, n):
        pl.semaphore_signal(
            barrier, inc=1, device_id={"ep": lax.rem(me + d, n)}, device_id_type=MESH
        )
    for d in range(1, nc):
        pl.semaphore_signal(
            barrier, inc=1, device_id={"corner": lax.rem(mc + d, nc)}, device_id_type=MESH
        )

    def send(src, dst, s_sem, r_sem, target):
        copy = pltpu.make_async_remote_copy(
            src_ref=src, dst_ref=dst, send_sem=s_sem, recv_sem=r_sem,
            device_id=target, device_id_type=MESH,
        )
        copy.start()
        return copy

    tables = make_tables(edges)
    sources = ((req, arr), (early, hreq))

    def smallest(step, carry):
        for kind, (plus, minus) in enumerate(sources):
            low = None
            for c in range(corners):
                at = pl.ds(corners * SUBS * step + c, SUBS, stride=corners)
                slack = plus[at, :] - minus[at, :]
                low = slack if low is None else jnp.minimum(low, slack)
            worst[pl.ds(2 * SUBS * step + kind, SUBS, stride=2), :] = low
        return carry

    lax.fori_loop(0, steps, smallest, 0, unroll=4)
    pl.semaphore_wait(barrier, n - 1 + nc - 1)

    def rows_of(k):
        return pl.ds(pl.multiple_of(k * share, SUBS), share)

    mins = []
    for d in range(1, nc):
        t = lax.rem(mc + d, nc)
        mins.append(send(worst.at[rows_of(t)], worst_in.at[d], ws.at[d], wr.at[d], {"corner": t}))

    def find(r):
        kind, c = r // corners, r % corners
        plus, minus = sources[kind]

        def body(step, low):
            at = pl.ds(corners * step + c, SUBS, stride=corners * steps)
            lanes = pl.ds(pl.multiple_of(step * LANES, LANES), LANES)
            slack = plus[at, :] - minus[at, :]
            part, even_at, odd_at, even, odd = search(tables, slack)
            group = ids[pl.ds(step, SUBS, stride=steps), :]
            codes[pl.ds(step, SUBS, stride=steps), :] = (part * GROUPS + group).astype(f32)
            for q, v in enumerate((even_at, odd_at)):
                marks[q, :, lanes] = v.astype(f32)
            marks[2, :, lanes] = even
            marks[3, :, lanes] = odd
            negative = jnp.minimum(slack, 0.0)
            coarse = negative.astype(narrow).astype(f32)
            over = jnp.where(even_at == 64, even, 0.0)
            for q, v in enumerate((over, coarse, negative - coarse)):
                tail[:, q, lanes] = v
            return jnp.minimum(low, slack)

        start = jnp.full((SUBS, LANES), jnp.inf, f32)
        low = lax.fori_loop(0, steps, body, start, unroll=4)
        low = jnp.min(jnp.min(low, axis=1, keepdims=True), axis=0, keepdims=True)
        least[r : r + 1] = jnp.broadcast_to(low, (1, LANES))

    iota = lax.broadcasted_iota(jnp.int32, (PACK, depth), 0).astype(f32).astype(narrow)
    zero = jnp.zeros((PACK, depth), narrow)
    width = 4 * GROUPS
    code_iota = lax.broadcasted_iota(jnp.int32, (LANES, width), 1).astype(f32).astype(narrow)
    code_zero = jnp.zeros((LANES, width), narrow)
    code_one = jnp.ones((LANES, width), narrow)

    def product(first, last):
        def body(s, carry):
            def spread(q):
                row = marks[q, pl.ds(s, 1), :]
                return jnp.broadcast_to(row, (PACK, depth)).astype(narrow)

            even_at, odd_at, even, odd = (spread(q) for q in range(FIELDS))
            left = []
            for at, v in ((even_at, even), (odd_at, odd)):
                for start in range(0, 64, PACK):
                    left.append(jnp.where(at == iota + narrow(start), v, zero))
            rest = jnp.concatenate([tail[s], jnp.zeros((SUBS, depth), f32)], axis=0)
            left.append(rest.astype(narrow))
            turned = codes[pl.ds(pl.multiple_of(s * steps, SUBS), steps), :].T.astype(narrow)
            right = []
            for t in range(steps):
                code = jnp.broadcast_to(turned[:, t : t + 1], (LANES, width))
                right.append(jnp.where(code == code_iota, code_one, code_zero))
            acc[...] += lax.dot_general(
                jnp.concatenate(left, axis=0),
                jnp.concatenate(right, axis=0),
                (((1,), (0,)), ((), ())),
                preferred_element_type=f32,
            )
            return carry

        lax.fori_loop(first, last, body, 0)

    lane = lax.broadcasted_iota(jnp.int32, (1, width), 1)

    def fold(v):
        v = v[:, :LANES] + v[:, LANES:]
        return v + pltpu.roll(jnp.broadcast_to(v, (SUBS, LANES)), GROUPS, 1)[0:1]

    def settle(r):
        full = acc[LANES : LANES + SUBS]
        over = pltpu.roll(jnp.broadcast_to(full[0:1], (SUBS, width)), GROUPS, 1)[0:1]
        acc[0:1] += jnp.where(lane >= GROUPS, over, 0.0)
        turned = acc[0:LANES].T
        for x in range(PAIR):
            for z in range(line):
                for g in range(4):
                    top = g * GROUPS + (x * line + z) * chunk
                    hist[r, x, z, :, g * LANES : (g + 1) * LANES] = turned[top : top + chunk]
        stats[r : r + 1] = fold(full[1:2] + full[2:3])
        if r == 0:
            stats[combos : combos + 1] = fold(full[3:4])

    def pair_of(z):
        return {"ep": z * PAIR + other}

    def line_of(z):
        return {"ep": z * PAIR + mx}

    weave_lane = lax.broadcasted_iota(jnp.int32, (chunk, LANES), 1)
    weave = (weave_lane >> 1) + (weave_lane & 1) * 64

    def finished(r, total):
        for g in range(4):
            at = slice(g * LANES, (g + 1) * LANES)
            hist_out[r, mine, :, at] = pick(total[:, at], weave) * density

    done = []

    def pair_send(r):
        return send(hist.at[r, other], pair_in.at[r], ps.at[r], pr.at[r], pair_of(mz))

    def line_send(r, copy):
        copy.wait_recv()
        hist[r, mx] += pair_in[r]
        copies = []
        for d in range(1, line):
            t = lax.rem(mz + d, line)
            copies.append(
                send(hist.at[r, mx, t], line_in.at[r, d], ls.at[r, d], lr.at[r, d], line_of(t))
            )
        done.append(copy)
        return copies

    def line_gather(r, copies):
        total = hist[r, mx, mz]
        for d in range(1, line):
            copies[d - 1].wait_recv()
            total += line_in[r, d]
        finished(r, total)
        part = hist_out.at[r, mine]
        back = [send(part, part, fs.at[r, 0], fr.at[r, 0], pair_of(mz))]
        for d in range(1, line):
            t = lax.rem(mz + d, line)
            back.append(send(part, part, gs.at[r, d], gr.at[r, d], line_of(t)))
        done.extend(copies)
        return back

    def forward(r, back):
        ends = [back[0]]
        for d in range(1, line):
            back[d].wait_recv()
            part = hist_out.at[r, mx * line + lax.rem(mz + line - d, line)]
            ends.append(send(part, part, fs.at[r, d], fr.at[r, d], pair_of(mz)))
        return back[1:], ends

    def all_send(r):
        copies = []
        for d in range(1, n):
            t = lax.rem(me + d, n)
            src = hist.at[r, lax.rem(t, PAIR), t // PAIR]
            copies.append(send(src, all_in.at[d], ls.at[r, d], lr.at[r, d], {"ep": t}))
        return copies

    def all_gather(r, copies):
        total = hist[r, mx, mz]
        for d in range(1, n):
            copies[d - 1].wait_recv()
            total += all_in[d]
        finished(r, total)
        part = hist_out.at[r, mine]
        back = []
        for d in range(1, n):
            t = lax.rem(me + d, n)
            back.append(send(part, part, gs.at[r, d], gr.at[r, d], {"ep": t}))
        done.extend(copies)
        return back

    row = lax.broadcasted_iota(jnp.int32, (SUBS, SUBS, depth), 1)
    tail[...] = jnp.where(row == 3, 1.0, 0.0).astype(f32)
    stats[...] = jnp.zeros_like(stats)

    paired, lined, backs, ended, all_sent = {}, {}, {}, {}, {}
    sent_only = []
    spread_out = []
    half = SUBS // 2

    def progress(slot):
        for action, r in plan.get(slot, ()):
            if action == "line":
                lined[r] = line_send(r, paired[r])
            elif action == "gather":
                backs[r] = line_gather(r, lined[r])
            elif action == "forward":
                got, ends = forward(r, backs[r])
                sent_only.extend(got)
                ended[r] = ends
            elif action == "worst":
                for copy in mins:
                    copy.wait_recv()
                low = worst[rows_of(mc)]
                for d in range(1, nc):
                    low = jnp.minimum(low, worst_in[d])
                worst_out[rows_of(mc)] = low
                for d in range(1, nc):
                    t = lax.rem(mc + d, nc)
                    part = worst_out.at[rows_of(mc)]
                    spread_out.append(send(part, part, vs.at[d], vr.at[d], {"corner": t}))

    for r in range(combos):
        find(r)
        acc[...] = jnp.zeros_like(acc)
        progress((r, 0))
        product(0, half)
        progress((r, 1))
        product(half, SUBS)
        settle(r)
        if r == combos - 1:
            all_sent[r] = all_send(r)
        else:
            paired[r] = pair_send(r)
        progress((r, 2))

    stats[combos * 2 : combos * 3] = least[0:combos]
    shares = []
    for d in range(1, n):
        t = lax.rem(me + d, n)
        shares.append(send(stats, stats_in.at[me], ss.at[d], sr.at[d], {"ep": t}))
    progress("end0")
    last = all_gather(combos - 1, all_sent[combos - 1])
    progress("end1")
    for copy in shares:
        copy.wait_recv()
    stats_in[me] = stats[...]
    added = stats_in[0, 0 : 2 * combos]
    lowest = stats_in[0, 2 * combos : 3 * combos]
    for k in range(1, n):
        added += stats_in[k, 0 : 2 * combos]
        lowest = jnp.minimum(lowest, stats_in[k, 2 * combos : 3 * combos])
    stats_out[0 : 2 * combos] = added
    stats_out[2 * combos : 3 * combos] = lowest
    for copy in spread_out + last:
        copy.wait_recv()
    for r in ended:
        for copy in ended[r]:
            copy.wait_recv()
    for copy in mins + done + sent_only + shares + spread_out + last:
        copy.wait_send()
    for r in ended:
        for copy in ended[r]:
            copy.wait_send()


def finish_kernel(endpoints, hist, stats, worst, hist_out, tns_out, share_out, total_out, least_out, worst_out):
    corners = total_out.shape[0]
    combos = 2 * corners
    share = GROUPS / endpoints
    for m in range(2):
        for c in range(corners):
            r = m * corners + c
            hist_out[:, c, m, :] = hist[r]
            row = stats[r : r + 1, :GROUPS]
            tns_out[c, m : m + 1, :] = row * share
            total = jnp.sum(row, axis=1, keepdims=True) * (1.0 / endpoints)
            total_out[c : c + 1, m : m + 1] = total
            least_out[c : c + 1, m : m + 1] = stats[2 * combos + r : 2 * combos + r + 1, 0:1]
    share_out[...] = stats[combos : combos + 1, :GROUPS] * share
    worst_out[...] = worst[...]


def make_plan(combos):
    plan = {(0, 1): [("worst", 0)]}
    for r in range(combos - 1):
        places = [(r + 1, 1), (r + 2, 0), (r + 2, 2)]
        for action, (q, part) in zip(("line", "gather", "forward"), places):
            key = (q, part) if q < combos else ("end0" if action == "gather" else "end1")
            plan.setdefault(key, []).append((action, r))
    return plan


def on_device(required, arrival, hold_required, early_arrival, part_ids, bin_edges):
    corners, rows = required.shape
    n, nc = lax.axis_size("ep"), lax.axis_size("corner")
    endpoints = rows * n
    bins = bin_edges.shape[0]
    combos = 2 * corners
    blocks = rows // LANES
    steps = blocks // SUBS
    depth = steps * LANES
    line = n // PAIR
    chunk = GROUPS // n
    f32 = jnp.float32

    def by_block(v):
        return v.reshape(corners, blocks, LANES).transpose(1, 0, 2).reshape(blocks * corners, LANES)

    vmem = pl.BlockSpec(memory_space=pltpu.VMEM)
    dma = pltpu.SemaphoreType.DMA
    hist, stats, worst = pl.pallas_call(
        functools.partial(report_kernel, n, nc, GROUPS * bins / endpoints, make_plan(combos)),
        out_shape=(
            jax.ShapeDtypeStruct((combos, n, chunk, bins), f32),
            jax.ShapeDtypeStruct((3 * combos, LANES), f32),
            jax.ShapeDtypeStruct((2 * blocks, LANES), f32),
        ),
        in_specs=[vmem] * 6,
        out_specs=[vmem] * 3,
        scratch_shapes=[
            pltpu.VMEM((FIELDS, SUBS, depth), f32),
            pltpu.VMEM((blocks, LANES), f32),
            pltpu.VMEM((SUBS, SUBS, depth), f32),
            pltpu.VMEM((LANES + PACK, 4 * GROUPS), f32),
            pltpu.VMEM((2 * blocks, LANES), f32),
            pltpu.VMEM((nc, 2 * blocks // nc, LANES), f32),
            pltpu.VMEM((combos, LANES), f32),
            pltpu.VMEM((combos, PAIR, line, chunk, bins), f32),
            pltpu.VMEM((combos, line, chunk, bins), f32),
            pltpu.VMEM((combos, line, chunk, bins), f32),
            pltpu.VMEM((n, chunk, bins), f32),
            pltpu.VMEM((3 * combos, LANES), f32),
            pltpu.VMEM((n, 3 * combos, LANES), f32),
        ]
        + [dma((combos,))] * 2
        + [dma((combos, n))] * 6
        + [dma((n,))] * 2
        + [dma((nc,))] * 4,
        compiler_params=pltpu.CompilerParams(collective_id=0, has_side_effects=True),
        name="report",
    )(
        by_block(required), by_block(arrival), by_block(hold_required), by_block(early_arrival),
        part_ids.reshape(blocks, LANES), bin_edges.reshape(bins // LANES, LANES),
    )
    worst = worst.reshape(blocks, 2, LANES).transpose(1, 0, 2).reshape(2, rows)
    part_hist, part_tns, part_share, tns, wns, worst = pl.pallas_call(
        functools.partial(finish_kernel, endpoints),
        out_shape=(
            jax.ShapeDtypeStruct((GROUPS, corners, 2, bins), f32),
            jax.ShapeDtypeStruct((corners, 2, GROUPS), f32),
            jax.ShapeDtypeStruct((1, GROUPS), f32),
            jax.ShapeDtypeStruct((corners, 2), f32),
            jax.ShapeDtypeStruct((corners, 2), f32),
            jax.ShapeDtypeStruct((2, rows), f32),
        ),
        in_specs=[vmem] * 3,
        out_specs=[vmem] * 6,
        name="finish",
    )(hist.reshape(combos, GROUPS, bins), stats, worst)
    return (part_hist, part_tns.transpose(2, 0, 1), part_share[0], tns, wns, worst)


def solution(mesh):
    in_specs = (
        P("corner", "ep"),
        P("corner", "ep"),
        P("corner", "ep"),
        P("corner", "ep"),
        P("ep"),
        P(),
    )
    out_specs = (
        P(None, "corner", None, None),
        P(None, "corner", None),
        P(),
        P("corner", None),
        P("corner", None),
        P(None, "ep"),
    )
    return jax.shard_map(
        on_device, mesh=mesh, in_specs=in_specs, out_specs=out_specs, check_vma=False
    )
```

```python
import functools
import jax
import jax.numpy as jnp
from jax import lax
from jax.experimental import pallas as pl
from jax.experimental.pallas import tpu as pltpu
from jax.sharding import PartitionSpec as P

GROUPS = 64
LANES = 128
SUBS = 8
SPAN = 32
PACK = 16
PAIR = 2
FIELDS = 4
MESH = pl.DeviceIdType.MESH


def pick(table, index):
    return jnp.take_along_axis(table, index, axis=1, mode="promise_in_bounds")


def make_tables(edges_ref):
    nodes = edges_ref[...].astype(jnp.float32) * 0.001
    lane = lax.broadcasted_iota(jnp.int32, (SUBS, LANES), 1)
    rows = [jnp.broadcast_to(nodes[q : q + 1], (SUBS, LANES)) for q in range(4)]

    def gathered(place):
        index = place & (LANES - 1)
        value = pick(rows[3], index)
        for q in (2, 1, 0):
            value = jnp.where(place < LANES * (q + 1), pick(rows[q], index), value)
        return value

    def same(row):
        return pick(row, jnp.zeros((SUBS, LANES), jnp.int32))

    steps = []
    for k in range(2, 8):
        steps.append(gathered(((lane << (9 - k)) + (1 << (8 - k))) & 511))
    last = [gathered(2 * lane + 1), gathered(2 * lane + 2 * LANES + 1)]
    return [same(row) for row in rows], steps, last


def search(tables, slack):
    quarter, steps, last = tables
    level = jnp.minimum(jnp.maximum(slack, quarter[0]), 0.0)
    top = level >= quarter[2]
    low = jnp.where(top, quarter[2], quarter[0])
    high = jnp.where(top, 0.0, quarter[2])
    value = jnp.where(top, quarter[3], quarter[1])
    above = level >= value
    low = jnp.where(above, value, low)
    high = jnp.where(above, high, value)
    index = jnp.where(top, 2, 0) + jnp.where(above, 1, 0)
    part = index
    for table in steps:
        value = pick(table, index)
        above = level >= value
        low = jnp.where(above, value, low)
        high = jnp.where(above, high, value)
        index = index + index
        index = jnp.where(above, index + 1, index)
    place = index & (LANES - 1)
    value = jnp.where(top, pick(last[1], place), pick(last[0], place))
    above = level >= value
    low = jnp.where(above, value, low)
    high = jnp.where(above, high, value)
    scale = 1.0 / (high - low)
    first = (high - level) * scale
    second = (level - low) * scale
    odd_at = index & 63
    even_at = jnp.where(above, odd_at + 1, odd_at)
    even = jnp.where(above, second, first)
    odd = jnp.where(above, first, second)
    return part, even_at, odd_at, even, odd


def report_kernel(
    n, nc, density, plan, accs,
    req, arr, hreq, early, ids, edges,
    hist_out, stats_out, worst_out,
    marks, codes, tail, acc, worst, worst_in, least,
    hist, pair_in, line_in, all_in, stats, stats_in,
    ps, pr, ls, lr, gs, gr, fs, fr, ss, sr, ws, wr, vs, vr,
):
    corners = hist.shape[0] // 2
    combos = 2 * corners
    blocks = ids.shape[0]
    steps = blocks // SUBS
    chunk = GROUPS // n
    line = n // PAIR
    share = worst_out.shape[0] // nc
    narrow = jnp.bfloat16
    f32 = jnp.float32
    me = lax.axis_index("ep")
    mc = lax.axis_index("corner")
    mx = lax.rem(me, PAIR)
    mz = me // PAIR
    other = PAIR - 1 - mx
    mine = mx * line + mz

    barrier = pltpu.get_barrier_semaphore()
    for d in range(1, n):
        pl.semaphore_signal(
            barrier, inc=1, device_id={"ep": lax.rem(me + d, n)}, device_id_type=MESH
        )
    for d in range(1, nc):
        pl.semaphore_signal(
            barrier, inc=1, device_id={"corner": lax.rem(mc + d, nc)}, device_id_type=MESH
        )

    def send(src, dst, s_sem, r_sem, target):
        copy = pltpu.make_async_remote_copy(
            src_ref=src, dst_ref=dst, send_sem=s_sem, recv_sem=r_sem,
            device_id=target, device_id_type=MESH,
        )
        copy.start()
        return copy

    tables = make_tables(edges)
    sources = ((req, arr), (early, hreq))

    def smallest(step, carry):
        for kind, (plus, minus) in enumerate(sources):
            low = None
            for c in range(corners):
                at = pl.ds(corners * SUBS * step + c, SUBS, stride=corners)
                slack = plus[at, :] - minus[at, :]
                low = slack if low is None else jnp.minimum(low, slack)
            worst[pl.ds(2 * SUBS * step + kind, SUBS, stride=2), :] = low
        return carry

    lax.fori_loop(0, steps, smallest, 0, unroll=4)
    pl.semaphore_wait(barrier, n - 1 + nc - 1)

    def rows_of(k):
        return pl.ds(pl.multiple_of(k * share, SUBS), share)

    mins = []
    for d in range(1, nc):
        t = lax.rem(mc + d, nc)
        mins.append(send(worst.at[rows_of(t)], worst_in.at[d], ws.at[d], wr.at[d], {"corner": t}))

    def find(r):
        kind, c = r // corners, r % corners
        plus, minus = sources[kind]

        def body(step, low):
            at = pl.ds(corners * SUBS * step + c, SUBS, stride=corners)
            here = pl.ds(pl.multiple_of(step * SUBS, SUBS), SUBS)
            slack = plus[at, :] - minus[at, :]
            part, even_at, odd_at, even, odd = search(tables, slack)
            codes[here, :] = (part * GROUPS + ids[here, :]).astype(f32)
            marks[0, here, :] = even_at.astype(f32)
            marks[1, here, :] = odd_at.astype(f32)
            marks[2, here, :] = even
            marks[3, here, :] = odd
            negative = jnp.minimum(slack, 0.0)
            coarse = negative.astype(narrow).astype(f32)
            over = jnp.where(even_at == 64, even, 0.0)
            for q, v in enumerate((over, coarse, negative - coarse)):
                tail[pl.ds(SUBS * SUBS * step + q, SUBS, stride=SUBS), :] = v
            return jnp.minimum(low, slack)

        start = jnp.full((SUBS, LANES), jnp.inf, f32)
        low = lax.fori_loop(0, steps, body, start, unroll=8)
        low = jnp.min(jnp.min(low, axis=1, keepdims=True), axis=0, keepdims=True)
        least[r : r + 1] = jnp.broadcast_to(low, (1, LANES))

    iota = lax.broadcasted_iota(jnp.int32, (PACK, LANES), 0).astype(f32).astype(narrow)
    zero = jnp.zeros((PACK, LANES), narrow)
    width = 4 * GROUPS
    code_iota = lax.broadcasted_iota(jnp.int32, (LANES, width), 1).astype(f32).astype(narrow)
    code_zero = jnp.zeros((LANES, width), narrow)
    code_one = jnp.ones((LANES, width), narrow)

    def product(first, last):
        def body(s, carry):
            base = pl.multiple_of(s * SPAN, SPAN)
            turned = codes[pl.ds(base, SPAN), :].T.astype(narrow)

            def left(t):
                def spread(q):
                    row = marks[q, pl.ds(base + t, 1), :]
                    return jnp.broadcast_to(row, (PACK, LANES)).astype(narrow)

                even_at, odd_at, even, odd = (spread(q) for q in range(FIELDS))
                parts = []
                for at, v in ((even_at, even), (odd_at, odd)):
                    for start in range(0, 64, PACK):
                        parts.append(jnp.where(at == iota + narrow(start), v, zero))
                rest = tail[pl.ds(pl.multiple_of(SUBS * (base + t), SUBS), SUBS), :]
                rest = jnp.concatenate([rest, jnp.zeros((SUBS, LANES), f32)], axis=0)
                return jnp.concatenate(parts + [rest.astype(narrow)], axis=0)

            def right(t):
                code = jnp.broadcast_to(turned[:, t : t + 1], (LANES, width))
                return jnp.where(code == code_iota, code_one, code_zero)

            def push(p):
                pltpu.matmul_push_rhs(
                    jnp.concatenate([right(2 * p), right(2 * p + 1)], axis=0),
                    staging_register=(p // 2) % 2, mxu_index=p % 2,
                )

            tiles = SPAN // 2
            push(0)
            push(1)
            for p in range(tiles):
                if p + 2 < tiles:
                    push(p + 2)
                pltpu.matmul_acc_lhs(
                    accs[p % 2],
                    jnp.concatenate([left(2 * p), left(2 * p + 1)], axis=1),
                    load_staged_rhs=(p // 2) % 2,
                )
            return carry

        lax.fori_loop(first, last, body, 0)

    lane = lax.broadcasted_iota(jnp.int32, (1, width), 1)

    def fold(v):
        v = v[:, :LANES] + v[:, LANES:]
        return v + pltpu.roll(jnp.broadcast_to(v, (SUBS, LANES)), GROUPS, 1)[0:1]

    def settle(r):
        acc[...] = pltpu.matmul_pop(accs[0]) + pltpu.matmul_pop(accs[1])
        full = acc[LANES : LANES + SUBS]
        over = pltpu.roll(jnp.broadcast_to(full[0:1], (SUBS, width)), GROUPS, 1)[0:1]
        acc[0:1] += jnp.where(lane >= GROUPS, over, 0.0)
        turned = acc[0:LANES].T
        for x in range(PAIR):
            for z in range(line):
                for g in range(4):
                    top = g * GROUPS + (x * line + z) * chunk
                    hist[r, x, z, :, g * LANES : (g + 1) * LANES] = turned[top : top + chunk]
        stats[r : r + 1] = fold(full[1:2] + full[2:3])
        if r == 0:
            stats[combos : combos + 1] = fold(full[3:4])

    def pair_of(z):
        return {"ep": z * PAIR + other}

    def line_of(z):
        return {"ep": z * PAIR + mx}

    weave_lane = lax.broadcasted_iota(jnp.int32, (chunk, LANES), 1)
    weave = (weave_lane >> 1) + (weave_lane & 1) * 64

    def finished(r, total):
        for g in range(4):
            at = slice(g * LANES, (g + 1) * LANES)
            hist_out[r, mine, :, at] = pick(total[:, at], weave) * density

    done = []

    def pair_send(r):
        return send(hist.at[r, other], pair_in.at[r], ps.at[r], pr.at[r], pair_of(mz))

    def line_send(r, copy):
        copy.wait_recv()
        hist[r, mx] += pair_in[r]
        copies = []
        for d in range(1, line):
            t = lax.rem(mz + d, line)
            copies.append(
                send(hist.at[r, mx, t], line_in.at[r, d], ls.at[r, d], lr.at[r, d], line_of(t))
            )
        done.append(copy)
        return copies

    def line_gather(r, copies):
        total = hist[r, mx, mz]
        for d in range(1, line):
            copies[d - 1].wait_recv()
            total += line_in[r, d]
        finished(r, total)
        part = hist_out.at[r, mine]
        back = [send(part, part, fs.at[r, 0], fr.at[r, 0], pair_of(mz))]
        for d in range(1, line):
            t = lax.rem(mz + d, line)
            back.append(send(part, part, gs.at[r, d], gr.at[r, d], line_of(t)))
        done.extend(copies)
        return back

    def forward(r, back):
        ends = [back[0]]
        for d in range(1, line):
            back[d].wait_recv()
            part = hist_out.at[r, mx * line + lax.rem(mz + line - d, line)]
            ends.append(send(part, part, fs.at[r, d], fr.at[r, d], pair_of(mz)))
        return back[1:], ends

    def all_send(r):
        copies = []
        for d in range(1, n):
            t = lax.rem(me + d, n)
            src = hist.at[r, lax.rem(t, PAIR), t // PAIR]
            copies.append(send(src, all_in.at[d], ls.at[r, d], lr.at[r, d], {"ep": t}))
        return copies

    def all_gather(r, copies):
        total = hist[r, mx, mz]
        for d in range(1, n):
            copies[d - 1].wait_recv()
            total += all_in[d]
        finished(r, total)
        part = hist_out.at[r, mine]
        back = []
        for d in range(1, n):
            t = lax.rem(me + d, n)
            back.append(send(part, part, gs.at[r, d], gr.at[r, d], {"ep": t}))
        done.extend(copies)
        return back

    row = lax.broadcasted_iota(jnp.int32, (SUBS, LANES), 0)
    fresh = jnp.where(row == 3, 1.0, 0.0).astype(f32)

    def clear(step, carry):
        tail[pl.ds(pl.multiple_of(SUBS * step, SUBS), SUBS), :] = fresh
        return carry

    lax.fori_loop(0, blocks, clear, 0, unroll=8)
    pltpu.matmul_pop(accs[0])
    pltpu.matmul_pop(accs[1])
    stats[...] = jnp.zeros_like(stats)

    paired, lined, backs, ended, all_sent = {}, {}, {}, {}, {}
    sent_only = []
    spread_out = []
    whole = blocks // SPAN
    half = whole // 2

    def progress(slot):
        for action, r in plan.get(slot, ()):
            if action == "line":
                lined[r] = line_send(r, paired[r])
            elif action == "gather":
                backs[r] = line_gather(r, lined[r])
            elif action == "forward":
                got, ends = forward(r, backs[r])
                sent_only.extend(got)
                ended[r] = ends
            elif action == "worst":
                for copy in mins:
                    copy.wait_recv()
                low = worst[rows_of(mc)]
                for d in range(1, nc):
                    low = jnp.minimum(low, worst_in[d])
                worst_out[rows_of(mc)] = low
                for d in range(1, nc):
                    t = lax.rem(mc + d, nc)
                    part = worst_out.at[rows_of(mc)]
                    spread_out.append(send(part, part, vs.at[d], vr.at[d], {"corner": t}))

    for r in range(combos):
        find(r)
        progress((r, 0))
        product(0, half)
        progress((r, 1))
        product(half, whole)
        settle(r)
        if r == combos - 1:
            all_sent[r] = all_send(r)
        else:
            paired[r] = pair_send(r)
        progress((r, 2))

    stats[combos * 2 : combos * 3] = least[0:combos]
    shares = []
    for d in range(1, n):
        t = lax.rem(me + d, n)
        shares.append(send(stats, stats_in.at[me], ss.at[d], sr.at[d], {"ep": t}))
    progress("end0")
    last = all_gather(combos - 1, all_sent[combos - 1])
    progress("end1")
    for copy in shares:
        copy.wait_recv()
    stats_in[me] = stats[...]
    added = stats_in[0, 0 : 2 * combos]
    lowest = stats_in[0, 2 * combos : 3 * combos]
    for k in range(1, n):
        added += stats_in[k, 0 : 2 * combos]
        lowest = jnp.minimum(lowest, stats_in[k, 2 * combos : 3 * combos])
    stats_out[0 : 2 * combos] = added
    stats_out[2 * combos : 3 * combos] = lowest
    for copy in spread_out + last:
        copy.wait_recv()
    for r in ended:
        for copy in ended[r]:
            copy.wait_recv()
    for copy in mins + done + sent_only + shares + spread_out + last:
        copy.wait_send()
    for r in ended:
        for copy in ended[r]:
            copy.wait_send()


def report(n, nc, density, plan, *refs):
    def body(first, second):
        report_kernel(n, nc, density, plan, (first, second), *refs)

    shape = (LANES + PACK, 4 * GROUPS)
    pl.run_scoped(body, pltpu.ACC(0)(shape, jnp.float32), pltpu.ACC(1)(shape, jnp.float32))


def finish_kernel(endpoints, hist, stats, worst, hist_out, tns_out, share_out, total_out, least_out, worst_out):
    corners = total_out.shape[0]
    combos = 2 * corners
    share = GROUPS / endpoints
    for m in range(2):
        for c in range(corners):
            r = m * corners + c
            hist_out[:, c, m, :] = hist[r]
            row = stats[r : r + 1, :GROUPS]
            tns_out[c, m : m + 1, :] = row * share
            total = jnp.sum(row, axis=1, keepdims=True) * (1.0 / endpoints)
            total_out[c : c + 1, m : m + 1] = total
            least_out[c : c + 1, m : m + 1] = stats[2 * combos + r : 2 * combos + r + 1, 0:1]
    share_out[...] = stats[combos : combos + 1, :GROUPS] * share
    worst_out[...] = worst[...]


def make_plan(combos):
    plan = {(0, 1): [("worst", 0)]}
    for r in range(combos - 1):
        places = [(r + 1, 1), (r + 2, 0), (r + 2, 2)]
        for action, (q, part) in zip(("line", "gather", "forward"), places):
            key = (q, part) if q < combos else ("end0" if action == "gather" else "end1")
            plan.setdefault(key, []).append((action, r))
    return plan


def on_device(required, arrival, hold_required, early_arrival, part_ids, bin_edges):
    corners, rows = required.shape
    n, nc = lax.axis_size("ep"), lax.axis_size("corner")
    endpoints = rows * n
    bins = bin_edges.shape[0]
    combos = 2 * corners
    blocks = rows // LANES
    line = n // PAIR
    chunk = GROUPS // n
    f32 = jnp.float32

    def by_block(v):
        return v.reshape(corners, blocks, LANES).transpose(1, 0, 2).reshape(blocks * corners, LANES)

    vmem = pl.BlockSpec(memory_space=pltpu.VMEM)
    dma = pltpu.SemaphoreType.DMA
    hist, stats, worst = pl.pallas_call(
        functools.partial(report, n, nc, GROUPS * bins / endpoints, make_plan(combos)),
        out_shape=(
            jax.ShapeDtypeStruct((combos, n, chunk, bins), f32),
            jax.ShapeDtypeStruct((3 * combos, LANES), f32),
            jax.ShapeDtypeStruct((2 * blocks, LANES), f32),
        ),
        in_specs=[vmem] * 6,
        out_specs=[vmem] * 3,
        scratch_shapes=[
            pltpu.VMEM((FIELDS, blocks, LANES), f32),
            pltpu.VMEM((blocks, LANES), f32),
            pltpu.VMEM((SUBS * blocks, LANES), f32),
            pltpu.VMEM((LANES + PACK, 4 * GROUPS), f32),
            pltpu.VMEM((2 * blocks, LANES), f32),
            pltpu.VMEM((nc, 2 * blocks // nc, LANES), f32),
            pltpu.VMEM((combos, LANES), f32),
            pltpu.VMEM((combos, PAIR, line, chunk, bins), f32),
            pltpu.VMEM((combos, line, chunk, bins), f32),
            pltpu.VMEM((combos, line, chunk, bins), f32),
            pltpu.VMEM((n, chunk, bins), f32),
            pltpu.VMEM((3 * combos, LANES), f32),
            pltpu.VMEM((n, 3 * combos, LANES), f32),
        ]
        + [dma((combos,))] * 2
        + [dma((combos, n))] * 6
        + [dma((n,))] * 2
        + [dma((nc,))] * 4,
        compiler_params=pltpu.CompilerParams(collective_id=0, has_side_effects=True),
        name="report",
    )(
        by_block(required), by_block(arrival), by_block(hold_required), by_block(early_arrival),
        part_ids.reshape(blocks, LANES), bin_edges.reshape(bins // LANES, LANES),
    )
    worst = worst.reshape(blocks, 2, LANES).transpose(1, 0, 2).reshape(2, rows)
    part_hist, part_tns, part_share, tns, wns, worst = pl.pallas_call(
        functools.partial(finish_kernel, endpoints),
        out_shape=(
            jax.ShapeDtypeStruct((GROUPS, corners, 2, bins), f32),
            jax.ShapeDtypeStruct((corners, 2, GROUPS), f32),
            jax.ShapeDtypeStruct((1, GROUPS), f32),
            jax.ShapeDtypeStruct((corners, 2), f32),
            jax.ShapeDtypeStruct((corners, 2), f32),
            jax.ShapeDtypeStruct((2, rows), f32),
        ),
        in_specs=[vmem] * 3,
        out_specs=[vmem] * 6,
        name="finish",
    )(hist.reshape(combos, GROUPS, bins), stats, worst)
    return (part_hist, part_tns.transpose(2, 0, 1), part_share[0], tns, wns, worst)


def solution(mesh):
    in_specs = (
        P("corner", "ep"),
        P("corner", "ep"),
        P("corner", "ep"),
        P("corner", "ep"),
        P("ep"),
        P(),
    )
    out_specs = (
        P(None, "corner", None, None),
        P(None, "corner", None),
        P(),
        P("corner", None),
        P("corner", None),
        P(None, "ep"),
    )
    return jax.shard_map(
        on_device, mesh=mesh, in_specs=in_specs, out_specs=out_specs, check_vma=False
    )
```

```python
import functools
import jax
import jax.numpy as jnp
from jax import lax
from jax.experimental import pallas as pl
from jax.experimental.pallas import tpu as pltpu
from jax.sharding import PartitionSpec as P

GROUPS = 64
LANES = 128
SUBS = 8
SPAN = 32
AHEAD = 4
PACK = 16
PAIR = 2
FIELDS = 4
MESH = pl.DeviceIdType.MESH


def pick(table, index):
    return jnp.take_along_axis(table, index, axis=1, mode="promise_in_bounds")


def make_tables(edges_ref):
    nodes = edges_ref[...].astype(jnp.float32) * 0.001
    lane = lax.broadcasted_iota(jnp.int32, (SUBS, LANES), 1)
    rows = [jnp.broadcast_to(nodes[q : q + 1], (SUBS, LANES)) for q in range(4)]

    def gathered(place):
        index = place & (LANES - 1)
        value = pick(rows[3], index)
        for q in (2, 1, 0):
            value = jnp.where(place < LANES * (q + 1), pick(rows[q], index), value)
        return value

    def same(row):
        return pick(row, jnp.zeros((SUBS, LANES), jnp.int32))

    eighths = [same(rows[k // 2]) if k % 2 == 0 else gathered(jnp.full((SUBS, LANES), 64 * k, jnp.int32)) for k in range(8)]
    steps = []
    for size in (16, 4, 1):
        steps.append([gathered((4 * size * lane + size * j) & 511) for j in (1, 2, 3)])
    return eighths, steps


def search(tables, slack):
    eighths, steps = tables
    level = jnp.minimum(jnp.maximum(slack, eighths[0]), 0.0)
    top = level >= eighths[4]
    low = jnp.where(top, eighths[4], eighths[0])
    high = jnp.where(top, 0.0, eighths[4])
    value = jnp.where(top, eighths[6], eighths[2])
    above = level >= value
    low = jnp.where(above, value, low)
    high = jnp.where(above, high, value)
    part = jnp.where(top, 2, 0) + jnp.where(above, 1, 0)
    value = jnp.where(
        top, jnp.where(above, eighths[7], eighths[5]), jnp.where(above, eighths[3], eighths[1])
    )
    above = level >= value
    low = jnp.where(above, value, low)
    high = jnp.where(above, high, value)
    index = part + part
    index = jnp.where(above, index + 1, index)
    for first_at, middle, last_at in steps:
        value = pick(middle, index)
        top = level >= value
        low = jnp.where(top, value, low)
        high = jnp.where(top, high, value)
        value = jnp.where(top, pick(last_at, index), pick(first_at, index))
        above = level >= value
        low = jnp.where(above, value, low)
        high = jnp.where(above, high, value)
        index = 4 * index
        index = jnp.where(top, index + 2, index)
        index = jnp.where(above, index + 1, index)
    scale = 1.0 / (high - low)
    first = (high - level) * scale
    second = (level - low) * scale
    odd_at = (index >> 1) & 63
    even_at = jnp.where(above, odd_at + 1, odd_at)
    even = jnp.where(above, second, first)
    odd = jnp.where(above, first, second)
    return part, even_at, odd_at, even, odd


def report_kernel(
    n, nc, density, plan, accs, spare,
    req, arr, hreq, early, ids, edges,
    hist_out, stats_out, worst_out,
    marks, codes, turned, tail, acc, worst, worst_in, least,
    hist, pair_in, line_in, all_in, stats, stats_in,
    ps, pr, ls, lr, gs, gr, fs, fr, ss, sr, ws, wr, vs, vr,
):
    corners = hist.shape[0] // 2
    combos = 2 * corners
    blocks = ids.shape[0]
    steps = blocks // SUBS
    chunk = GROUPS // n
    line = n // PAIR
    share = worst_out.shape[0] // nc
    narrow = jnp.bfloat16
    f32 = jnp.float32
    me = lax.axis_index("ep")
    mc = lax.axis_index("corner")
    mx = lax.rem(me, PAIR)
    mz = me // PAIR
    other = PAIR - 1 - mx
    mine = mx * line + mz

    barrier = pltpu.get_barrier_semaphore()
    for d in range(1, n):
        pl.semaphore_signal(
            barrier, inc=1, device_id={"ep": lax.rem(me + d, n)}, device_id_type=MESH
        )
    for d in range(1, nc):
        pl.semaphore_signal(
            barrier, inc=1, device_id={"corner": lax.rem(mc + d, nc)}, device_id_type=MESH
        )

    def send(src, dst, s_sem, r_sem, target):
        copy = pltpu.make_async_remote_copy(
            src_ref=src, dst_ref=dst, send_sem=s_sem, recv_sem=r_sem,
            device_id=target, device_id_type=MESH,
        )
        copy.start()
        return copy

    tables = make_tables(edges)
    sources = ((req, arr), (early, hreq))

    def smallest(step, carry):
        for kind, (plus, minus) in enumerate(sources):
            low = None
            for c in range(corners):
                at = pl.ds(corners * SUBS * step + c, SUBS, stride=corners)
                slack = plus[at, :] - minus[at, :]
                low = slack if low is None else jnp.minimum(low, slack)
            worst[pl.ds(2 * SUBS * step + kind, SUBS, stride=2), :] = low
        return carry

    lax.fori_loop(0, steps, smallest, 0, unroll=4)
    pl.semaphore_wait(barrier, n - 1 + nc - 1)

    def rows_of(k):
        return pl.ds(pl.multiple_of(k * share, SUBS), share)

    mins = []
    for d in range(1, nc):
        t = lax.rem(mc + d, nc)
        mins.append(send(worst.at[rows_of(t)], worst_in.at[d], ws.at[d], wr.at[d], {"corner": t}))

    def find(r):
        kind, c = r // corners, r % corners
        plus, minus = sources[kind]

        def body(step, low):
            at = pl.ds(corners * SUBS * step + c, SUBS, stride=corners)
            here = pl.ds(pl.multiple_of(step * SUBS, SUBS), SUBS)
            slack = plus[at, :] - minus[at, :]
            part, even_at, odd_at, even, odd = search(tables, slack)
            codes[here, :] = (part * GROUPS + ids[here, :]).astype(f32)
            marks[0, here, :] = even_at.astype(f32)
            marks[1, here, :] = odd_at.astype(f32)
            marks[2, here, :] = even
            marks[3, here, :] = odd
            negative = jnp.minimum(slack, 0.0)
            coarse = negative.astype(narrow).astype(f32)
            over = jnp.where(even_at == 64, even, 0.0)
            for q, v in enumerate((over, coarse, negative - coarse)):
                tail[pl.ds(SUBS * SUBS * step + q, SUBS, stride=SUBS), :] = v
            return jnp.minimum(low, slack)

        start = jnp.full((SUBS, LANES), jnp.inf, f32)
        low = lax.fori_loop(0, steps, body, start, unroll=8)
        low = jnp.min(jnp.min(low, axis=1, keepdims=True), axis=0, keepdims=True)
        least[r : r + 1] = jnp.broadcast_to(low, (1, LANES))
        for s in range(blocks // SPAN):
            turned[s, :, :SPAN] = codes[s * SPAN : (s + 1) * SPAN].T

    iota = lax.broadcasted_iota(jnp.int32, (PACK, LANES), 0).astype(f32).astype(narrow)
    zero = jnp.zeros((PACK, LANES), narrow)
    width = 4 * GROUPS
    code_iota = lax.broadcasted_iota(jnp.int32, (LANES, width), 1).astype(f32).astype(narrow)
    code_zero = jnp.zeros((LANES, width), narrow)
    code_one = jnp.ones((LANES, width), narrow)

    tiles = SPAN // 2
    whole = blocks // SPAN

    def push(columns, p):
        parts = []
        for t in (2 * p, 2 * p + 1):
            code = jnp.broadcast_to(columns[:, t : t + 1], (LANES, width))
            parts.append(jnp.where(code == code_iota, code_one, code_zero))
        pltpu.matmul_push_rhs(
            jnp.concatenate(parts, axis=0), staging_register=(p // 2) % 2, mxu_index=p % 2
        )

    def left(at):
        def spread(q):
            row = marks[q, pl.ds(at, 1), :]
            return jnp.broadcast_to(row, (PACK, LANES)).astype(narrow)

        even_at, odd_at, even, odd = (spread(q) for q in range(FIELDS))
        parts = []
        for place, v in ((even_at, even), (odd_at, odd)):
            for start in range(0, 64, PACK):
                parts.append(jnp.where(place == iota + narrow(start), v, zero))
        rest = tail[pl.ds(pl.multiple_of(SUBS * at, SUBS), SUBS), :]
        rest = jnp.concatenate([rest, jnp.zeros((SUBS, LANES), f32)], axis=0)
        return jnp.concatenate(parts + [rest.astype(narrow)], axis=0)

    def begin():
        columns = turned[0, :, :SPAN].astype(narrow)
        for p in range(AHEAD):
            push(columns, p)

    def product(first, last):
        def body(s, carry):
            base = pl.multiple_of(s * SPAN, SPAN)
            columns = turned[s, :, :SPAN].astype(narrow)
            later = turned[jnp.minimum(s + 1, whole - 1), :, :SPAN].astype(narrow)
            for p in range(tiles):
                pltpu.matmul_acc_lhs(
                    accs[p % 2],
                    jnp.concatenate([left(base + 2 * p), left(base + 2 * p + 1)], axis=1),
                    load_staged_rhs=(p // 2) % 2,
                )
                if p + AHEAD < tiles:
                    push(columns, p + AHEAD)
                else:
                    push(later, p + AHEAD - tiles)
            return carry

        lax.fori_loop(first, last, body, 0)

    def drain():
        nothing = jnp.zeros((PACK, width), narrow)
        for p in range(AHEAD):
            pltpu.matmul_acc_lhs(spare[p % 2], nothing, load_staged_rhs=(p // 2) % 2)

    lane = lax.broadcasted_iota(jnp.int32, (1, width), 1)

    def fold(v):
        v = v[:, :LANES] + v[:, LANES:]
        return v + pltpu.roll(jnp.broadcast_to(v, (SUBS, LANES)), GROUPS, 1)[0:1]

    def settle(r):
        drain()
        acc[...] = pltpu.matmul_pop(accs[0]) + pltpu.matmul_pop(accs[1])
        full = acc[LANES : LANES + SUBS]
        over = pltpu.roll(jnp.broadcast_to(full[0:1], (SUBS, width)), GROUPS, 1)[0:1]
        acc[0:1] += jnp.where(lane >= GROUPS, over, 0.0)
        turned = acc[0:LANES].T
        for x in range(PAIR):
            for z in range(line):
                for g in range(4):
                    top = g * GROUPS + (x * line + z) * chunk
                    hist[r, x, z, :, g * LANES : (g + 1) * LANES] = turned[top : top + chunk]
        stats[r : r + 1] = fold(full[1:2] + full[2:3])
        if r == 0:
            stats[combos : combos + 1] = fold(full[3:4])

    def pair_of(z):
        return {"ep": z * PAIR + other}

    def line_of(z):
        return {"ep": z * PAIR + mx}

    weave_lane = lax.broadcasted_iota(jnp.int32, (chunk, LANES), 1)
    weave = (weave_lane >> 1) + (weave_lane & 1) * 64

    def finished(r, total):
        for g in range(4):
            at = slice(g * LANES, (g + 1) * LANES)
            hist_out[r, mine, :, at] = pick(total[:, at], weave) * density

    done = []

    def pair_send(r):
        return send(hist.at[r, other], pair_in.at[r], ps.at[r], pr.at[r], pair_of(mz))

    def line_send(r, copy):
        copy.wait_recv()
        hist[r, mx] += pair_in[r]
        copies = []
        for d in range(1, line):
            t = lax.rem(mz + d, line)
            copies.append(
                send(hist.at[r, mx, t], line_in.at[r, d], ls.at[r, d], lr.at[r, d], line_of(t))
            )
        done.append(copy)
        return copies

    def line_gather(r, copies):
        total = hist[r, mx, mz]
        for d in range(1, line):
            copies[d - 1].wait_recv()
            total += line_in[r, d]
        finished(r, total)
        part = hist_out.at[r, mine]
        back = [send(part, part, fs.at[r, 0], fr.at[r, 0], pair_of(mz))]
        for d in range(1, line):
            t = lax.rem(mz + d, line)
            back.append(send(part, part, gs.at[r, d], gr.at[r, d], line_of(t)))
        done.extend(copies)
        return back

    def forward(r, back):
        ends = [back[0]]
        for d in range(1, line):
            back[d].wait_recv()
            part = hist_out.at[r, mx * line + lax.rem(mz + line - d, line)]
            ends.append(send(part, part, fs.at[r, d], fr.at[r, d], pair_of(mz)))
        return back[1:], ends

    def all_send(r):
        copies = []
        for d in range(1, n):
            t = lax.rem(me + d, n)
            src = hist.at[r, lax.rem(t, PAIR), t // PAIR]
            copies.append(send(src, all_in.at[d], ls.at[r, d], lr.at[r, d], {"ep": t}))
        return copies

    def all_gather(r, copies):
        total = hist[r, mx, mz]
        for d in range(1, n):
            copies[d - 1].wait_recv()
            total += all_in[d]
        finished(r, total)
        part = hist_out.at[r, mine]
        back = []
        for d in range(1, n):
            t = lax.rem(me + d, n)
            back.append(send(part, part, gs.at[r, d], gr.at[r, d], {"ep": t}))
        done.extend(copies)
        return back

    row = lax.broadcasted_iota(jnp.int32, (SUBS, LANES), 0)
    fresh = jnp.where(row == 3, 1.0, 0.0).astype(f32)

    def clear(step, carry):
        tail[pl.ds(pl.multiple_of(SUBS * step, SUBS), SUBS), :] = fresh
        return carry

    lax.fori_loop(0, blocks, clear, 0, unroll=8)
    pltpu.matmul_pop(accs[0])
    pltpu.matmul_pop(accs[1])
    pltpu.matmul_pop(spare[0])
    pltpu.matmul_pop(spare[1])
    stats[...] = jnp.zeros_like(stats)

    paired, lined, backs, ended, all_sent = {}, {}, {}, {}, {}
    sent_only = []
    spread_out = []
    half = whole // 2

    def progress(slot):
        for action, r in plan.get(slot, ()):
            if action == "line":
                lined[r] = line_send(r, paired[r])
            elif action == "gather":
                backs[r] = line_gather(r, lined[r])
            elif action == "forward":
                got, ends = forward(r, backs[r])
                sent_only.extend(got)
                ended[r] = ends
            elif action == "worst":
                for copy in mins:
                    copy.wait_recv()
                low = worst[rows_of(mc)]
                for d in range(1, nc):
                    low = jnp.minimum(low, worst_in[d])
                worst_out[rows_of(mc)] = low
                for d in range(1, nc):
                    t = lax.rem(mc + d, nc)
                    part = worst_out.at[rows_of(mc)]
                    spread_out.append(send(part, part, vs.at[d], vr.at[d], {"corner": t}))

    for r in range(combos):
        find(r)
        begin()
        progress((r, 0))
        product(0, half)
        progress((r, 1))
        product(half, whole)
        settle(r)
        if r == combos - 1:
            all_sent[r] = all_send(r)
        else:
            paired[r] = pair_send(r)
        progress((r, 2))

    stats[combos * 2 : combos * 3] = least[0:combos]
    shares = []
    for d in range(1, n):
        t = lax.rem(me + d, n)
        shares.append(send(stats, stats_in.at[me], ss.at[d], sr.at[d], {"ep": t}))
    progress("end0")
    last = all_gather(combos - 1, all_sent[combos - 1])
    progress("end1")
    for copy in shares:
        copy.wait_recv()
    stats_in[me] = stats[...]
    added = stats_in[0, 0 : 2 * combos]
    lowest = stats_in[0, 2 * combos : 3 * combos]
    for k in range(1, n):
        added += stats_in[k, 0 : 2 * combos]
        lowest = jnp.minimum(lowest, stats_in[k, 2 * combos : 3 * combos])
    stats_out[0 : 2 * combos] = added
    stats_out[2 * combos : 3 * combos] = lowest
    for copy in spread_out + last:
        copy.wait_recv()
    for r in ended:
        for copy in ended[r]:
            copy.wait_recv()
    for copy in mins + done + sent_only + shares + spread_out + last:
        copy.wait_send()
    for r in ended:
        for copy in ended[r]:
            copy.wait_send()


def report(n, nc, density, plan, *refs):
    def body(*units):
        report_kernel(n, nc, density, plan, units[:2], units[2:], *refs)

    units = [
        pltpu.ACC(q)((rows, 4 * GROUPS), jnp.float32)
        for rows in (LANES + PACK, PACK)
        for q in range(2)
    ]
    pl.run_scoped(body, *units)


def finish_kernel(endpoints, hist, stats, worst, hist_out, tns_out, share_out, total_out, least_out, worst_out):
    corners = total_out.shape[0]
    combos = 2 * corners
    share = GROUPS / endpoints
    for m in range(2):
        for c in range(corners):
            r = m * corners + c
            hist_out[:, c, m, :] = hist[r]
            row = stats[r : r + 1, :GROUPS]
            tns_out[c, m : m + 1, :] = row * share
            total = jnp.sum(row, axis=1, keepdims=True) * (1.0 / endpoints)
            total_out[c : c + 1, m : m + 1] = total
            least_out[c : c + 1, m : m + 1] = stats[2 * combos + r : 2 * combos + r + 1, 0:1]
    share_out[...] = stats[combos : combos + 1, :GROUPS] * share
    worst_out[...] = worst[...]


def make_plan(combos):
    plan = {(0, 1): [("worst", 0)]}
    for r in range(combos - 1):
        places = [(r + 1, 1), (r + 2, 0), (r + 2, 2)]
        for action, (q, part) in zip(("line", "gather", "forward"), places):
            key = (q, part) if q < combos else ("end0" if action == "gather" else "end1")
            plan.setdefault(key, []).append((action, r))
    return plan


def on_device(required, arrival, hold_required, early_arrival, part_ids, bin_edges):
    corners, rows = required.shape
    n, nc = lax.axis_size("ep"), lax.axis_size("corner")
    endpoints = rows * n
    bins = bin_edges.shape[0]
    combos = 2 * corners
    blocks = rows // LANES
    line = n // PAIR
    chunk = GROUPS // n
    f32 = jnp.float32

    def by_block(v):
        return v.reshape(corners, blocks, LANES).transpose(1, 0, 2).reshape(blocks * corners, LANES)

    vmem = pl.BlockSpec(memory_space=pltpu.VMEM)
    dma = pltpu.SemaphoreType.DMA
    hist, stats, worst = pl.pallas_call(
        functools.partial(report, n, nc, GROUPS * bins / endpoints, make_plan(combos)),
        out_shape=(
            jax.ShapeDtypeStruct((combos, n, chunk, bins), f32),
            jax.ShapeDtypeStruct((3 * combos, LANES), f32),
            jax.ShapeDtypeStruct((2 * blocks, LANES), f32),
        ),
        in_specs=[vmem] * 6,
        out_specs=[vmem] * 3,
        scratch_shapes=[
            pltpu.VMEM((FIELDS, blocks, LANES), f32),
            pltpu.VMEM((blocks, LANES), f32),
            pltpu.VMEM((blocks // SPAN, LANES, LANES), f32),
            pltpu.VMEM((SUBS * blocks, LANES), f32),
            pltpu.VMEM((LANES + PACK, 4 * GROUPS), f32),
            pltpu.VMEM((2 * blocks, LANES), f32),
            pltpu.VMEM((nc, 2 * blocks // nc, LANES), f32),
            pltpu.VMEM((combos, LANES), f32),
            pltpu.VMEM((combos, PAIR, line, chunk, bins), f32),
            pltpu.VMEM((combos, line, chunk, bins), f32),
            pltpu.VMEM((combos, line, chunk, bins), f32),
            pltpu.VMEM((n, chunk, bins), f32),
            pltpu.VMEM((3 * combos, LANES), f32),
            pltpu.VMEM((n, 3 * combos, LANES), f32),
        ]
        + [dma((combos,))] * 2
        + [dma((combos, n))] * 6
        + [dma((n,))] * 2
        + [dma((nc,))] * 4,
        compiler_params=pltpu.CompilerParams(collective_id=0, has_side_effects=True),
        name="report",
    )(
        by_block(required), by_block(arrival), by_block(hold_required), by_block(early_arrival),
        part_ids.reshape(blocks, LANES), bin_edges.reshape(bins // LANES, LANES),
    )
    worst = worst.reshape(blocks, 2, LANES).transpose(1, 0, 2).reshape(2, rows)
    part_hist, part_tns, part_share, tns, wns, worst = pl.pallas_call(
        functools.partial(finish_kernel, endpoints),
        out_shape=(
            jax.ShapeDtypeStruct((GROUPS, corners, 2, bins), f32),
            jax.ShapeDtypeStruct((corners, 2, GROUPS), f32),
            jax.ShapeDtypeStruct((1, GROUPS), f32),
            jax.ShapeDtypeStruct((corners, 2), f32),
            jax.ShapeDtypeStruct((corners, 2), f32),
            jax.ShapeDtypeStruct((2, rows), f32),
        ),
        in_specs=[vmem] * 3,
        out_specs=[vmem] * 6,
        name="finish",
    )(hist.reshape(combos, GROUPS, bins), stats, worst)
    return (part_hist, part_tns.transpose(2, 0, 1), part_share[0], tns, wns, worst)


def solution(mesh):
    in_specs = (
        P("corner", "ep"),
        P("corner", "ep"),
        P("corner", "ep"),
        P("corner", "ep"),
        P("ep"),
        P(),
    )
    out_specs = (
        P(None, "corner", None, None),
        P(None, "corner", None),
        P(),
        P("corner", None),
        P("corner", None),
        P(None, "ep"),
    )
    return jax.shard_map(
        on_device, mesh=mesh, in_specs=in_specs, out_specs=out_specs, check_vma=False
    )
```

```python
import functools
import jax
import jax.numpy as jnp
from jax import lax
from jax.experimental import pallas as pl
from jax.experimental.pallas import tpu as pltpu
from jax.sharding import PartitionSpec as P

GROUPS = 64
LANES = 128
SUBS = 8
SPAN = 32
AHEAD = 4
PACK = 16
PAIR = 2
FIELDS = 4
MESH = pl.DeviceIdType.MESH


def pick(table, index):
    return jnp.take_along_axis(table, index, axis=1, mode="promise_in_bounds")


def make_tables(edges_ref):
    nodes = edges_ref[...].astype(jnp.float32) * 0.001
    lane = lax.broadcasted_iota(jnp.int32, (SUBS, LANES), 1)
    rows = [jnp.broadcast_to(nodes[q : q + 1], (SUBS, LANES)) for q in range(4)]

    def gathered(place):
        index = place & (LANES - 1)
        value = pick(rows[3], index)
        for q in (2, 1, 0):
            value = jnp.where(place < LANES * (q + 1), pick(rows[q], index), value)
        return value

    def same(row):
        return pick(row, jnp.zeros((SUBS, LANES), jnp.int32))

    eighths = [same(rows[k // 2]) if k % 2 == 0 else gathered(jnp.full((SUBS, LANES), 64 * k, jnp.int32)) for k in range(8)]
    steps = []
    for size in (16, 4, 1):
        steps.append([gathered((4 * size * lane + size * j) & 511) for j in (1, 2, 3)])
    return eighths, steps


def search(tables, slack):
    eighths, steps = tables
    level = jnp.minimum(jnp.maximum(slack, eighths[0]), 0.0)
    top = level >= eighths[4]
    low = jnp.where(top, eighths[4], eighths[0])
    high = jnp.where(top, 0.0, eighths[4])
    value = jnp.where(top, eighths[6], eighths[2])
    above = level >= value
    low = jnp.where(above, value, low)
    high = jnp.where(above, high, value)
    part = jnp.where(top, 2, 0) + jnp.where(above, 1, 0)
    value = jnp.where(
        top, jnp.where(above, eighths[7], eighths[5]), jnp.where(above, eighths[3], eighths[1])
    )
    above = level >= value
    low = jnp.where(above, value, low)
    high = jnp.where(above, high, value)
    index = part + part
    index = jnp.where(above, index + 1, index)
    for first_at, middle, last_at in steps:
        value = pick(middle, index)
        top = level >= value
        low = jnp.where(top, value, low)
        high = jnp.where(top, high, value)
        value = jnp.where(top, pick(last_at, index), pick(first_at, index))
        above = level >= value
        low = jnp.where(above, value, low)
        high = jnp.where(above, high, value)
        index = 4 * index
        index = jnp.where(top, index + 2, index)
        index = jnp.where(above, index + 1, index)
    scale = 1.0 / (high - low)
    first = (high - level) * scale
    second = (level - low) * scale
    odd_at = (index >> 1) & 63
    even_at = jnp.where(above, odd_at + 1, odd_at)
    even = jnp.where(above, second, first)
    odd = jnp.where(above, first, second)
    return part, even_at, odd_at, even, odd


def report_kernel(
    n, nc, density, plan, accs, spare,
    req_hbm, arr_hbm, hreq_hbm, early_hbm, ids_hbm, edges_hbm,
    hist_out, stats_out, worst_out,
    req, arr, hreq, early, ids, edges, into,
    marks, codes, turned, tail, acc, worst, worst_in, least,
    hist, pair_in, line_in, all_in, stats, stats_in,
    ps, pr, ls, lr, gs, gr, fs, fr, ss, sr, ws, wr, vs, vr,
):
    corners = hist.shape[0] // 2
    combos = 2 * corners
    blocks = ids.shape[0]
    steps = blocks // SUBS
    chunk = GROUPS // n
    line = n // PAIR
    share = worst_out.shape[0] // nc
    narrow = jnp.bfloat16
    f32 = jnp.float32
    me = lax.axis_index("ep")
    mc = lax.axis_index("corner")
    mx = lax.rem(me, PAIR)
    mz = me // PAIR
    other = PAIR - 1 - mx
    mine = mx * line + mz

    loads = []
    for k, (src, dst) in enumerate((
        (edges_hbm, edges), (req_hbm, req), (arr_hbm, arr), (ids_hbm, ids), (early_hbm, early), (hreq_hbm, hreq)
    )):
        loads.append(pltpu.make_async_copy(src, dst, into.at[k]))
        loads[-1].start()

    barrier = pltpu.get_barrier_semaphore()
    for d in range(1, n):
        pl.semaphore_signal(
            barrier, inc=1, device_id={"ep": lax.rem(me + d, n)}, device_id_type=MESH
        )
    for d in range(1, nc):
        pl.semaphore_signal(
            barrier, inc=1, device_id={"corner": lax.rem(mc + d, nc)}, device_id_type=MESH
        )

    def send(src, dst, s_sem, r_sem, target):
        copy = pltpu.make_async_remote_copy(
            src_ref=src, dst_ref=dst, send_sem=s_sem, recv_sem=r_sem,
            device_id=target, device_id_type=MESH,
        )
        copy.start()
        return copy

    def rows_of(k):
        return pl.ds(pl.multiple_of(k * share, SUBS), share)

    row = lax.broadcasted_iota(jnp.int32, (SUBS, LANES), 0)
    fresh = jnp.where(row == 3, 1.0, 0.0).astype(f32)

    def clear(step, carry):
        tail[pl.ds(pl.multiple_of(SUBS * step, SUBS), SUBS), :] = fresh
        return carry

    lax.fori_loop(0, blocks, clear, 0, unroll=8)
    loads[0].wait()
    tables = make_tables(edges)
    sources = ((req, arr), (early, hreq))

    mins = []

    def share_worst():
        def smallest(step, carry):
            for kind, (plus, minus) in enumerate(sources):
                low = None
                for c in range(corners):
                    at = pl.ds(corners * SUBS * step + c, SUBS, stride=corners)
                    slack = plus[at, :] - minus[at, :]
                    low = slack if low is None else jnp.minimum(low, slack)
                worst[pl.ds(2 * SUBS * step + kind, SUBS, stride=2), :] = low
            return carry

        lax.fori_loop(0, steps, smallest, 0, unroll=4)
        pl.semaphore_wait(barrier, n - 1 + nc - 1)
        for d in range(1, nc):
            t = lax.rem(mc + d, nc)
            mins.append(send(worst.at[rows_of(t)], worst_in.at[d], ws.at[d], wr.at[d], {"corner": t}))

    def find(r):
        kind, c = r // corners, r % corners
        plus, minus = sources[kind]

        def body(step, low):
            at = pl.ds(corners * SUBS * step + c, SUBS, stride=corners)
            here = pl.ds(pl.multiple_of(step * SUBS, SUBS), SUBS)
            slack = plus[at, :] - minus[at, :]
            part, even_at, odd_at, even, odd = search(tables, slack)
            codes[here, :] = (part * GROUPS + ids[here, :]).astype(f32)
            marks[0, here, :] = even_at.astype(f32)
            marks[1, here, :] = odd_at.astype(f32)
            marks[2, here, :] = even
            marks[3, here, :] = odd
            negative = jnp.minimum(slack, 0.0)
            coarse = negative.astype(narrow).astype(f32)
            over = jnp.where(even_at == 64, even, 0.0)
            for q, v in enumerate((over, coarse, negative - coarse)):
                tail[pl.ds(SUBS * SUBS * step + q, SUBS, stride=SUBS), :] = v
            return jnp.minimum(low, slack)

        start = jnp.full((SUBS, LANES), jnp.inf, f32)
        low = lax.fori_loop(0, steps, body, start, unroll=8)
        low = jnp.min(jnp.min(low, axis=1, keepdims=True), axis=0, keepdims=True)
        least[r : r + 1] = jnp.broadcast_to(low, (1, LANES))
        for s in range(blocks // SPAN):
            turned[s, :, :SPAN] = codes[s * SPAN : (s + 1) * SPAN].T

    iota = lax.broadcasted_iota(jnp.int32, (PACK, LANES), 0).astype(f32).astype(narrow)
    zero = jnp.zeros((PACK, LANES), narrow)
    width = 4 * GROUPS
    code_iota = lax.broadcasted_iota(jnp.int32, (LANES, width), 1).astype(f32).astype(narrow)
    code_zero = jnp.zeros((LANES, width), narrow)
    code_one = jnp.ones((LANES, width), narrow)

    tiles = SPAN // 2
    whole = blocks // SPAN

    def push(columns, p):
        parts = []
        for t in (2 * p, 2 * p + 1):
            code = jnp.broadcast_to(columns[:, t : t + 1], (LANES, width))
            parts.append(jnp.where(code == code_iota, code_one, code_zero))
        pltpu.matmul_push_rhs(
            jnp.concatenate(parts, axis=0), staging_register=(p // 2) % 2, mxu_index=p % 2
        )

    def left(at):
        def spread(q):
            row = marks[q, pl.ds(at, 1), :]
            return jnp.broadcast_to(row, (PACK, LANES)).astype(narrow)

        even_at, odd_at, even, odd = (spread(q) for q in range(FIELDS))
        parts = []
        for place, v in ((even_at, even), (odd_at, odd)):
            for start in range(0, 64, PACK):
                parts.append(jnp.where(place == iota + narrow(start), v, zero))
        rest = tail[pl.ds(pl.multiple_of(SUBS * at, SUBS), SUBS), :]
        rest = jnp.concatenate([rest, jnp.zeros((SUBS, LANES), f32)], axis=0)
        return jnp.concatenate(parts + [rest.astype(narrow)], axis=0)

    def begin():
        columns = turned[0, :, :SPAN].astype(narrow)
        for p in range(AHEAD):
            push(columns, p)

    def product(first, last):
        def body(s, carry):
            base = pl.multiple_of(s * SPAN, SPAN)
            columns = turned[s, :, :SPAN].astype(narrow)
            later = turned[jnp.minimum(s + 1, whole - 1), :, :SPAN].astype(narrow)
            for p in range(tiles):
                pltpu.matmul_acc_lhs(
                    accs[p % 2],
                    jnp.concatenate([left(base + 2 * p), left(base + 2 * p + 1)], axis=1),
                    load_staged_rhs=(p // 2) % 2,
                )
                if p + AHEAD < tiles:
                    push(columns, p + AHEAD)
                else:
                    push(later, p + AHEAD - tiles)
            return carry

        lax.fori_loop(first, last, body, 0)

    def drain():
        nothing = jnp.zeros((PACK, width), narrow)
        for p in range(AHEAD):
            pltpu.matmul_acc_lhs(spare[p % 2], nothing, load_staged_rhs=(p // 2) % 2)

    lane = lax.broadcasted_iota(jnp.int32, (1, width), 1)

    def fold(v):
        v = v[:, :LANES] + v[:, LANES:]
        return v + pltpu.roll(jnp.broadcast_to(v, (SUBS, LANES)), GROUPS, 1)[0:1]

    def settle(r):
        drain()
        acc[...] = pltpu.matmul_pop(accs[0]) + pltpu.matmul_pop(accs[1])
        full = acc[LANES : LANES + SUBS]
        over = pltpu.roll(jnp.broadcast_to(full[0:1], (SUBS, width)), GROUPS, 1)[0:1]
        acc[0:1] += jnp.where(lane >= GROUPS, over, 0.0)
        turned = acc[0:LANES].T
        for x in range(PAIR):
            for z in range(line):
                for g in range(4):
                    top = g * GROUPS + (x * line + z) * chunk
                    hist[r, x, z, :, g * LANES : (g + 1) * LANES] = turned[top : top + chunk]
        stats[r : r + 1] = fold(full[1:2] + full[2:3])
        if r == 0:
            stats[combos : combos + 1] = fold(full[3:4])

    def pair_of(z):
        return {"ep": z * PAIR + other}

    def line_of(z):
        return {"ep": z * PAIR + mx}

    weave_lane = lax.broadcasted_iota(jnp.int32, (chunk, LANES), 1)
    weave = (weave_lane >> 1) + (weave_lane & 1) * 64

    def finished(r, total):
        for g in range(4):
            at = slice(g * LANES, (g + 1) * LANES)
            hist_out[r, mine, :, at] = pick(total[:, at], weave) * density

    done = []

    def pair_send(r):
        return send(hist.at[r, other], pair_in.at[r], ps.at[r], pr.at[r], pair_of(mz))

    def line_send(r, copy):
        copy.wait_recv()
        hist[r, mx] += pair_in[r]
        copies = []
        for d in range(1, line):
            t = lax.rem(mz + d, line)
            copies.append(
                send(hist.at[r, mx, t], line_in.at[r, d], ls.at[r, d], lr.at[r, d], line_of(t))
            )
        done.append(copy)
        return copies

    def line_gather(r, copies):
        total = hist[r, mx, mz]
        for d in range(1, line):
            copies[d - 1].wait_recv()
            total += line_in[r, d]
        finished(r, total)
        part = hist_out.at[r, mine]
        back = [send(part, part, fs.at[r, 0], fr.at[r, 0], pair_of(mz))]
        for d in range(1, line):
            t = lax.rem(mz + d, line)
            back.append(send(part, part, gs.at[r, d], gr.at[r, d], line_of(t)))
        done.extend(copies)
        return back

    def forward(r, back):
        ends = [back[0]]
        for d in range(1, line):
            back[d].wait_recv()
            part = hist_out.at[r, mx * line + lax.rem(mz + line - d, line)]
            ends.append(send(part, part, fs.at[r, d], fr.at[r, d], pair_of(mz)))
        return back[1:], ends

    def all_send(r):
        copies = []
        for d in range(1, n):
            t = lax.rem(me + d, n)
            src = hist.at[r, lax.rem(t, PAIR), t // PAIR]
            copies.append(send(src, all_in.at[d], ls.at[r, d], lr.at[r, d], {"ep": t}))
        return copies

    def all_gather(r, copies):
        total = hist[r, mx, mz]
        for d in range(1, n):
            copies[d - 1].wait_recv()
            total += all_in[d]
        finished(r, total)
        part = hist_out.at[r, mine]
        back = []
        for d in range(1, n):
            t = lax.rem(me + d, n)
            back.append(send(part, part, gs.at[r, d], gr.at[r, d], {"ep": t}))
        done.extend(copies)
        return back

    pltpu.matmul_pop(accs[0])
    pltpu.matmul_pop(accs[1])
    pltpu.matmul_pop(spare[0])
    pltpu.matmul_pop(spare[1])
    stats[...] = jnp.zeros_like(stats)

    paired, lined, backs, ended, all_sent = {}, {}, {}, {}, {}
    sent_only = []
    spread_out = []
    half = whole // 2

    def progress(slot):
        for action, r in plan.get(slot, ()):
            if action == "line":
                lined[r] = line_send(r, paired[r])
            elif action == "gather":
                backs[r] = line_gather(r, lined[r])
            elif action == "forward":
                got, ends = forward(r, backs[r])
                sent_only.extend(got)
                ended[r] = ends
            elif action == "worst":
                for copy in mins:
                    copy.wait_recv()
                low = worst[rows_of(mc)]
                for d in range(1, nc):
                    low = jnp.minimum(low, worst_in[d])
                worst_out[rows_of(mc)] = low
                for d in range(1, nc):
                    t = lax.rem(mc + d, nc)
                    part = worst_out.at[rows_of(mc)]
                    spread_out.append(send(part, part, vs.at[d], vr.at[d], {"corner": t}))

    for r in range(combos):
        if r == 0:
            for load in loads[1:4]:
                load.wait()
        find(r)
        if r == 0:
            for load in loads[4:]:
                load.wait()
            share_worst()
        begin()
        progress((r, 0))
        product(0, half)
        progress((r, 1))
        product(half, whole)
        settle(r)
        if r == combos - 1:
            all_sent[r] = all_send(r)
        else:
            paired[r] = pair_send(r)
        progress((r, 2))

    stats[combos * 2 : combos * 3] = least[0:combos]
    shares = []
    for d in range(1, n):
        t = lax.rem(me + d, n)
        shares.append(send(stats, stats_in.at[me], ss.at[d], sr.at[d], {"ep": t}))
    progress("end0")
    last = all_gather(combos - 1, all_sent[combos - 1])
    progress("end1")
    for copy in shares:
        copy.wait_recv()
    stats_in[me] = stats[...]
    added = stats_in[0, 0 : 2 * combos]
    lowest = stats_in[0, 2 * combos : 3 * combos]
    for k in range(1, n):
        added += stats_in[k, 0 : 2 * combos]
        lowest = jnp.minimum(lowest, stats_in[k, 2 * combos : 3 * combos])
    stats_out[0 : 2 * combos] = added
    stats_out[2 * combos : 3 * combos] = lowest
    for copy in spread_out + last:
        copy.wait_recv()
    for r in ended:
        for copy in ended[r]:
            copy.wait_recv()
    for copy in mins + done + sent_only + shares + spread_out + last:
        copy.wait_send()
    for r in ended:
        for copy in ended[r]:
            copy.wait_send()


def report(n, nc, density, plan, *refs):
    def body(*units):
        report_kernel(n, nc, density, plan, units[:2], units[2:], *refs)

    units = [
        pltpu.ACC(q)((rows, 4 * GROUPS), jnp.float32)
        for rows in (LANES + PACK, PACK)
        for q in range(2)
    ]
    pl.run_scoped(body, *units)


def finish_kernel(endpoints, hist, stats, worst, hist_out, tns_out, share_out, total_out, least_out, worst_out):
    corners = total_out.shape[0]
    combos = 2 * corners
    share = GROUPS / endpoints
    for m in range(2):
        for c in range(corners):
            r = m * corners + c
            hist_out[:, c, m, :] = hist[r]
            row = stats[r : r + 1, :GROUPS]
            tns_out[c, m : m + 1, :] = row * share
            total = jnp.sum(row, axis=1, keepdims=True) * (1.0 / endpoints)
            total_out[c : c + 1, m : m + 1] = total
            least_out[c : c + 1, m : m + 1] = stats[2 * combos + r : 2 * combos + r + 1, 0:1]
    share_out[...] = stats[combos : combos + 1, :GROUPS] * share
    for j in range(worst.shape[0] // 2):
        worst_out[:, j * LANES : (j + 1) * LANES] = worst[2 * j : 2 * j + 2, :]


def make_plan(combos):
    plan = {(1, 0): [("worst", 0)]}
    for r in range(combos - 1):
        places = [(r + 1, 1), (r + 2, 0), (r + 2, 2)]
        for action, (q, part) in zip(("line", "gather", "forward"), places):
            key = (q, part) if q < combos else ("end0" if action == "gather" else "end1")
            plan.setdefault(key, []).append((action, r))
    return plan


def on_device(required, arrival, hold_required, early_arrival, part_ids, bin_edges):
    corners, rows = required.shape
    n, nc = lax.axis_size("ep"), lax.axis_size("corner")
    endpoints = rows * n
    bins = bin_edges.shape[0]
    combos = 2 * corners
    blocks = rows // LANES
    line = n // PAIR
    chunk = GROUPS // n
    f32 = jnp.float32

    def by_block(v):
        return v.reshape(corners, blocks, LANES).transpose(1, 0, 2).reshape(blocks * corners, LANES)

    vmem = pl.BlockSpec(memory_space=pltpu.VMEM)
    dma = pltpu.SemaphoreType.DMA
    hist, stats, worst = pl.pallas_call(
        functools.partial(report, n, nc, GROUPS * bins / endpoints, make_plan(combos)),
        out_shape=(
            jax.ShapeDtypeStruct((combos, n, chunk, bins), f32),
            jax.ShapeDtypeStruct((3 * combos, LANES), f32),
            jax.ShapeDtypeStruct((2 * blocks, LANES), f32),
        ),
        in_specs=[pl.BlockSpec(memory_space=pltpu.HBM)] * 6,
        out_specs=[vmem] * 3,
        scratch_shapes=[pltpu.VMEM((corners * blocks, LANES), f32)] * 4
        + [
            pltpu.VMEM((blocks, LANES), jnp.int32),
            pltpu.VMEM((bins // LANES, LANES), jnp.int32),
            dma((6,)),
            pltpu.VMEM((FIELDS, blocks, LANES), f32),
            pltpu.VMEM((blocks, LANES), f32),
            pltpu.VMEM((blocks // SPAN, LANES, LANES), f32),
            pltpu.VMEM((SUBS * blocks, LANES), f32),
            pltpu.VMEM((LANES + PACK, 4 * GROUPS), f32),
            pltpu.VMEM((2 * blocks, LANES), f32),
            pltpu.VMEM((nc, 2 * blocks // nc, LANES), f32),
            pltpu.VMEM((combos, LANES), f32),
            pltpu.VMEM((combos, PAIR, line, chunk, bins), f32),
            pltpu.VMEM((combos, line, chunk, bins), f32),
            pltpu.VMEM((combos, line, chunk, bins), f32),
            pltpu.VMEM((n, chunk, bins), f32),
            pltpu.VMEM((3 * combos, LANES), f32),
            pltpu.VMEM((n, 3 * combos, LANES), f32),
        ]
        + [dma((combos,))] * 2
        + [dma((combos, n))] * 6
        + [dma((n,))] * 2
        + [dma((nc,))] * 4,
        compiler_params=pltpu.CompilerParams(
            collective_id=0, has_side_effects=True, vmem_limit_bytes=24 * 1024 * 1024
        ),
        name="report",
    )(
        *[
            pltpu.with_memory_space_constraint(v, pltpu.HBM)
            for v in (
                by_block(required), by_block(arrival), by_block(hold_required),
                by_block(early_arrival), part_ids.reshape(blocks, LANES),
                bin_edges.reshape(bins // LANES, LANES),
            )
        ]
    )
    part_hist, part_tns, part_share, tns, wns, worst = pl.pallas_call(
        functools.partial(finish_kernel, endpoints),
        out_shape=(
            jax.ShapeDtypeStruct((GROUPS, corners, 2, bins), f32),
            jax.ShapeDtypeStruct((corners, 2, GROUPS), f32),
            jax.ShapeDtypeStruct((1, GROUPS), f32),
            jax.ShapeDtypeStruct((corners, 2), f32),
            jax.ShapeDtypeStruct((corners, 2), f32),
            jax.ShapeDtypeStruct((2, rows), f32),
        ),
        in_specs=[vmem] * 3,
        out_specs=[vmem] * 6,
        compiler_params=pltpu.CompilerParams(vmem_limit_bytes=8 * 1024 * 1024),
        name="finish",
    )(hist.reshape(combos, GROUPS, bins), stats, worst)
    return (part_hist, part_tns.transpose(2, 0, 1), part_share[0], tns, wns, worst)


def solution(mesh):
    in_specs = (
        P("corner", "ep"),
        P("corner", "ep"),
        P("corner", "ep"),
        P("corner", "ep"),
        P("ep"),
        P(),
    )
    out_specs = (
        P(None, "corner", None, None),
        P(None, "corner", None),
        P(),
        P("corner", None),
        P("corner", None),
        P(None, "ep"),
    )
    return jax.shard_map(
        on_device, mesh=mesh, in_specs=in_specs, out_specs=out_specs, check_vma=False
    )
```

```python
import functools
import jax
import jax.numpy as jnp
from jax import lax
from jax.experimental import pallas as pl
from jax.experimental.pallas import tpu as pltpu
from jax.sharding import PartitionSpec as P

GROUPS = 64
LANES = 128
SUBS = 8
SPAN = 128
AHEAD = 4
PACK = 16
PAIR = 2
FIELDS = 4
MESH = pl.DeviceIdType.MESH


def pick(table, index):
    return jnp.take_along_axis(table, index, axis=1, mode="promise_in_bounds")


def make_tables(edges_ref):
    nodes = edges_ref[...].astype(jnp.float32) * 0.001
    lane = lax.broadcasted_iota(jnp.int32, (SUBS, LANES), 1)
    rows = [jnp.broadcast_to(nodes[q : q + 1], (SUBS, LANES)) for q in range(4)]

    def gathered(place):
        index = place & (LANES - 1)
        value = pick(rows[3], index)
        for q in (2, 1, 0):
            value = jnp.where(place < LANES * (q + 1), pick(rows[q], index), value)
        return value

    def same(row):
        return pick(row, jnp.zeros((SUBS, LANES), jnp.int32))

    eighths = [same(rows[k // 2]) if k % 2 == 0 else gathered(jnp.full((SUBS, LANES), 64 * k, jnp.int32)) for k in range(8)]
    steps = []
    for size in (16, 4, 1):
        steps.append([gathered((4 * size * lane + size * j) & 511) for j in (1, 2, 3)])
    return eighths, steps


def search(tables, slack):
    eighths, steps = tables
    level = jnp.minimum(jnp.maximum(slack, eighths[0]), 0.0)
    top = level >= eighths[4]
    low = jnp.where(top, eighths[4], eighths[0])
    high = jnp.where(top, 0.0, eighths[4])
    value = jnp.where(top, eighths[6], eighths[2])
    above = level >= value
    low = jnp.where(above, value, low)
    high = jnp.where(above, high, value)
    part = jnp.where(top, 2, 0) + jnp.where(above, 1, 0)
    value = jnp.where(
        top, jnp.where(above, eighths[7], eighths[5]), jnp.where(above, eighths[3], eighths[1])
    )
    above = level >= value
    low = jnp.where(above, value, low)
    high = jnp.where(above, high, value)
    index = part + part
    index = jnp.where(above, index + 1, index)
    for first_at, middle, last_at in steps:
        value = pick(middle, index)
        top = level >= value
        low = jnp.where(top, value, low)
        high = jnp.where(top, high, value)
        value = jnp.where(top, pick(last_at, index), pick(first_at, index))
        above = level >= value
        low = jnp.where(above, value, low)
        high = jnp.where(above, high, value)
        index = 4 * index
        index = jnp.where(top, index + 2, index)
        index = jnp.where(above, index + 1, index)
    scale = 1.0 / (high - low)
    first = (high - level) * scale
    second = (level - low) * scale
    odd_at = (index >> 1) & 63
    even_at = jnp.where(above, odd_at + 1, odd_at)
    even = jnp.where(above, second, first)
    odd = jnp.where(above, first, second)
    return part, even_at, odd_at, even, odd


def report_kernel(
    n, nc, density, plan, accs, spare,
    req_hbm, arr_hbm, hreq_hbm, early_hbm, ids_hbm, edges_hbm,
    hist_out, stats_out, worst_out,
    req, arr, hreq, early, ids, edges, into,
    marks, codes, turned, tail, acc, worst, worst_in, least,
    hist, all_in, stats, stats_in,
    ls, lr, gs, gr, fs, fr, ss, sr, ws, wr, vs, vr,
):
    corners = hist.shape[0] // 2
    combos = 2 * corners
    blocks = ids.shape[0]
    steps = blocks // SUBS
    chunk = GROUPS // n
    line = n // PAIR
    share = worst_out.shape[0] // nc
    narrow = jnp.bfloat16
    f32 = jnp.float32
    me = lax.axis_index("ep")
    mc = lax.axis_index("corner")
    mx = lax.rem(me, PAIR)
    mz = me // PAIR
    other = PAIR - 1 - mx
    mine = mx * line + mz

    loads = []
    for k, (src, dst) in enumerate((
        (edges_hbm, edges), (req_hbm, req), (arr_hbm, arr), (ids_hbm, ids), (early_hbm, early), (hreq_hbm, hreq)
    )):
        loads.append(pltpu.make_async_copy(src, dst, into.at[k]))
        loads[-1].start()

    barrier = pltpu.get_barrier_semaphore()
    for d in range(1, n):
        pl.semaphore_signal(
            barrier, inc=1, device_id={"ep": lax.rem(me + d, n)}, device_id_type=MESH
        )
    for d in range(1, nc):
        pl.semaphore_signal(
            barrier, inc=1, device_id={"corner": lax.rem(mc + d, nc)}, device_id_type=MESH
        )

    def send(src, dst, s_sem, r_sem, target):
        copy = pltpu.make_async_remote_copy(
            src_ref=src, dst_ref=dst, send_sem=s_sem, recv_sem=r_sem,
            device_id=target, device_id_type=MESH,
        )
        copy.start()
        return copy

    def rows_of(k):
        return pl.ds(pl.multiple_of(k * share, SUBS), share)

    row = lax.broadcasted_iota(jnp.int32, (SUBS, LANES), 0)
    fresh = jnp.where(row == 3, 1.0, 0.0).astype(f32)

    def clear(step, carry):
        tail[pl.ds(pl.multiple_of(SUBS * step, SUBS), SUBS), :] = fresh
        return carry

    lax.fori_loop(0, blocks, clear, 0, unroll=8)
    loads[0].wait()
    tables = make_tables(edges)
    sources = ((req, arr), (early, hreq))

    mins = []

    def share_worst():
        def smallest(step, carry):
            for kind, (plus, minus) in enumerate(sources):
                low = None
                for c in range(corners):
                    at = pl.ds(corners * SUBS * step + c, SUBS, stride=corners)
                    slack = plus[at, :] - minus[at, :]
                    low = slack if low is None else jnp.minimum(low, slack)
                worst[pl.ds(2 * SUBS * step + kind, SUBS, stride=2), :] = low
            return carry

        lax.fori_loop(0, steps, smallest, 0, unroll=4)
        pl.semaphore_wait(barrier, n - 1 + nc - 1)
        for d in range(1, nc):
            t = lax.rem(mc + d, nc)
            mins.append(send(worst.at[rows_of(t)], worst_in.at[d], ws.at[d], wr.at[d], {"corner": t}))

    def find(r):
        kind, c = r // corners, r % corners
        plus, minus = sources[kind]

        def body(step, low):
            at = pl.ds(corners * SUBS * step + c, SUBS, stride=corners)
            here = pl.ds(pl.multiple_of(step * SUBS, SUBS), SUBS)
            slack = plus[at, :] - minus[at, :]
            part, even_at, odd_at, even, odd = search(tables, slack)
            codes[here, :] = (part * GROUPS + ids[here, :]).astype(f32)
            marks[0, here, :] = even_at.astype(f32)
            marks[1, here, :] = odd_at.astype(f32)
            marks[2, here, :] = even
            marks[3, here, :] = odd
            negative = jnp.minimum(slack, 0.0)
            coarse = negative.astype(narrow).astype(f32)
            over = jnp.where(even_at == 64, even, 0.0)
            for q, v in enumerate((over, coarse, negative - coarse)):
                tail[pl.ds(SUBS * SUBS * step + q, SUBS, stride=SUBS), :] = v
            return jnp.minimum(low, slack)

        start = jnp.full((SUBS, LANES), jnp.inf, f32)
        low = lax.fori_loop(0, steps, body, start, unroll=16)
        low = jnp.min(jnp.min(low, axis=1, keepdims=True), axis=0, keepdims=True)
        least[r : r + 1] = jnp.broadcast_to(low, (1, LANES))
        for s in range(blocks // SPAN):
            turned[s, :, :SPAN] = codes[s * SPAN : (s + 1) * SPAN].T

    iota = lax.broadcasted_iota(jnp.int32, (PACK, LANES), 0).astype(f32).astype(narrow)
    zero = jnp.zeros((PACK, LANES), narrow)
    width = 4 * GROUPS
    code_iota = lax.broadcasted_iota(jnp.int32, (LANES, width), 1).astype(f32).astype(narrow)
    code_zero = jnp.zeros((LANES, width), narrow)
    code_one = jnp.ones((LANES, width), narrow)

    tiles = SPAN // 2
    whole = blocks // SPAN

    def push(columns, p):
        parts = []
        for t in (2 * p, 2 * p + 1):
            code = jnp.broadcast_to(columns[:, t : t + 1], (LANES, width))
            parts.append(jnp.where(code == code_iota, code_one, code_zero))
        pltpu.matmul_push_rhs(
            jnp.concatenate(parts, axis=0), staging_register=(p // 2) % 2, mxu_index=p % 2
        )

    def left(at):
        def spread(q):
            row = marks[q, pl.ds(at, 1), :]
            return jnp.broadcast_to(row, (PACK, LANES)).astype(narrow)

        even_at, odd_at, even, odd = (spread(q) for q in range(FIELDS))
        parts = []
        for place, v in ((even_at, even), (odd_at, odd)):
            for start in range(0, 64, PACK):
                parts.append(jnp.where(place == iota + narrow(start), v, zero))
        rest = tail[pl.ds(pl.multiple_of(SUBS * at, SUBS), SUBS), :]
        rest = jnp.concatenate([rest, jnp.zeros((SUBS, LANES), f32)], axis=0)
        return jnp.concatenate(parts + [rest.astype(narrow)], axis=0)

    def begin():
        columns = turned[0, :, :SPAN].astype(narrow)
        for p in range(AHEAD):
            push(columns, p)

    def product(first, last):
        def body(s, carry):
            base = pl.multiple_of(s * SPAN, SPAN)
            columns = turned[s, :, :SPAN].astype(narrow)
            later = turned[jnp.minimum(s + 1, whole - 1), :, :SPAN].astype(narrow)
            for p in range(tiles):
                pltpu.matmul_acc_lhs(
                    accs[p % 2],
                    jnp.concatenate([left(base + 2 * p), left(base + 2 * p + 1)], axis=1),
                    load_staged_rhs=(p // 2) % 2,
                )
                if p + AHEAD < tiles:
                    push(columns, p + AHEAD)
                else:
                    push(later, p + AHEAD - tiles)
            return carry

        lax.fori_loop(first, last, body, 0)

    def drain():
        nothing = jnp.zeros((PACK, width), narrow)
        for p in range(AHEAD):
            pltpu.matmul_acc_lhs(spare[p % 2], nothing, load_staged_rhs=(p // 2) % 2)

    lane = lax.broadcasted_iota(jnp.int32, (1, width), 1)

    def fold(v):
        v = v[:, :LANES] + v[:, LANES:]
        return v + pltpu.roll(jnp.broadcast_to(v, (SUBS, LANES)), GROUPS, 1)[0:1]

    def settle(r):
        drain()
        acc[...] = pltpu.matmul_pop(accs[0]) + pltpu.matmul_pop(accs[1])
        full = acc[LANES : LANES + SUBS]
        over = pltpu.roll(jnp.broadcast_to(full[0:1], (SUBS, width)), GROUPS, 1)[0:1]
        acc[0:1] += jnp.where(lane >= GROUPS, over, 0.0)
        turned = acc[0:LANES].T
        for x in range(PAIR):
            for z in range(line):
                for g in range(4):
                    top = g * GROUPS + (x * line + z) * chunk
                    hist[r, x, z, :, g * LANES : (g + 1) * LANES] = turned[top : top + chunk]
        stats[r : r + 1] = fold(full[1:2] + full[2:3])
        if r == 0:
            stats[combos : combos + 1] = fold(full[3:4])

    def pair_of(z):
        return {"ep": z * PAIR + other}

    def line_of(z):
        return {"ep": z * PAIR + mx}

    weave_lane = lax.broadcasted_iota(jnp.int32, (chunk, LANES), 1)
    weave = (weave_lane >> 1) + (weave_lane & 1) * 64

    done = []

    def all_send(r):
        copies = []
        for d in range(1, n):
            t = lax.rem(me + d, n)
            src = hist.at[r, lax.rem(t, PAIR), t // PAIR]
            copies.append(send(src, all_in.at[r, d], ls.at[r, d], lr.at[r, d], {"ep": t}))
        return copies

    def all_sum(r, copies):
        total = hist[r, mx, mz]
        for d in range(1, n):
            copies[d - 1].wait_recv()
            total += all_in[r, d]
        for g in range(total.shape[1] // LANES):
            at = slice(g * LANES, (g + 1) * LANES)
            hist_out[r, mine, :, at] = pick(total[:, at], weave) * density
        done.extend(copies)

    def all_gather(r, copies):
        all_sum(r, copies)
        part = hist_out.at[r, mine]
        back = []
        for d in range(1, n):
            t = lax.rem(me + d, n)
            back.append(send(part, part, gs.at[r, d], gr.at[r, d], {"ep": t}))
        return back

    def line_gather(r, copies):
        all_sum(r, copies)
        part = hist_out.at[r, mine]
        back = [send(part, part, fs.at[r, 0], fr.at[r, 0], pair_of(mz))]
        for d in range(1, line):
            t = lax.rem(mz + d, line)
            back.append(send(part, part, gs.at[r, d], gr.at[r, d], line_of(t)))
        return back

    def forward(r, back):
        ends = [back[0]]
        for d in range(1, line):
            back[d].wait_recv()
            part = hist_out.at[r, mx * line + lax.rem(mz + line - d, line)]
            ends.append(send(part, part, fs.at[r, d], fr.at[r, d], pair_of(mz)))
        return back[1:], ends

    pltpu.matmul_pop(accs[0])
    pltpu.matmul_pop(accs[1])
    pltpu.matmul_pop(spare[0])
    pltpu.matmul_pop(spare[1])
    stats[...] = jnp.zeros_like(stats)

    backs, ended, all_sent = {}, {}, {}
    sent_only = []
    spread_out = []
    half = whole // 2

    def progress(slot):
        for action, r in plan.get(slot, ()):
            if action == "all":
                all_sent[r] = all_send(r)
            elif action == "all_gather":
                ended[r] = all_gather(r, all_sent[r])
            elif action == "line_gather":
                backs[r] = line_gather(r, all_sent[r])
            elif action == "forward":
                got, ends = forward(r, backs[r])
                sent_only.extend(got)
                ended[r] = ends
            elif action == "worst":
                for copy in mins:
                    copy.wait_recv()
                low = worst[rows_of(mc)]
                for d in range(1, nc):
                    low = jnp.minimum(low, worst_in[d])
                worst_out[rows_of(mc)] = low
                for d in range(1, nc):
                    t = lax.rem(mc + d, nc)
                    part = worst_out.at[rows_of(mc)]
                    spread_out.append(send(part, part, vs.at[d], vr.at[d], {"corner": t}))

    for r in range(combos):
        if r == 0:
            for load in loads[1:4]:
                load.wait()
        find(r)
        if r == 0:
            for load in loads[4:]:
                load.wait()
            share_worst()
        begin()
        progress((r, 0))
        product(0, half)
        progress((r, 1))
        product(half, whole)
        settle(r)
        progress((r, 2))

    stats[combos * 2 : combos * 3] = least[0:combos]
    shares = []
    for d in range(1, n):
        t = lax.rem(me + d, n)
        shares.append(send(stats, stats_in.at[me], ss.at[d], sr.at[d], {"ep": t}))
    progress("end")
    for copy in shares:
        copy.wait_recv()
    stats_in[me] = stats[...]
    added = stats_in[0, 0 : 2 * combos]
    lowest = stats_in[0, 2 * combos : 3 * combos]
    for k in range(1, n):
        added += stats_in[k, 0 : 2 * combos]
        lowest = jnp.minimum(lowest, stats_in[k, 2 * combos : 3 * combos])
    stats_out[0 : 2 * combos] = added
    stats_out[2 * combos : 3 * combos] = lowest
    for copy in spread_out:
        copy.wait_recv()
    for r in ended:
        for copy in ended[r]:
            copy.wait_recv()
    for copy in mins + done + sent_only + shares + spread_out:
        copy.wait_send()
    for r in ended:
        for copy in ended[r]:
            copy.wait_send()


def report(n, nc, density, plan, *refs):
    def body(*units):
        report_kernel(n, nc, density, plan, units[:2], units[2:], *refs)

    units = [
        pltpu.ACC(q)((rows, 4 * GROUPS), jnp.float32)
        for rows in (LANES + PACK, PACK)
        for q in range(2)
    ]
    pl.run_scoped(body, *units)


def finish_kernel(endpoints, hist, stats, worst, hist_out, tns_out, share_out, total_out, least_out, worst_out):
    corners = total_out.shape[0]
    combos = 2 * corners
    share = GROUPS / endpoints
    for m in range(2):
        for c in range(corners):
            r = m * corners + c
            hist_out[:, c, m, :] = hist[r]
            row = stats[r : r + 1, :GROUPS]
            tns_out[c, m : m + 1, :] = row * share
            total = jnp.sum(row, axis=1, keepdims=True) * (1.0 / endpoints)
            total_out[c : c + 1, m : m + 1] = total
            least_out[c : c + 1, m : m + 1] = stats[2 * combos + r : 2 * combos + r + 1, 0:1]
    share_out[...] = stats[combos : combos + 1, :GROUPS] * share
    for j in range(worst.shape[0] // 2):
        worst_out[:, j * LANES : (j + 1) * LANES] = worst[2 * j : 2 * j + 2, :]


def make_plan(combos):
    last = combos - 1
    plan = {(1, 0): [("worst", 0)], "end": []}
    for r in range(combos):
        plan[r, 2] = [("all", r)]
        gather = [("line_gather", r)] if r < last else [("all_gather", r)]
        if r < last - 1:
            plan[r + 2, 0] = gather
            if r > 0:
                plan[r + 2, 0].append(("forward", r - 1))
        else:
            if r == last and last > 1:
                plan["end"].append(("forward", last - 2))
            plan["end"] += gather
    plan["end"].append(("forward", last - 1))
    return plan


def on_device(required, arrival, hold_required, early_arrival, part_ids, bin_edges):
    corners, rows = required.shape
    n, nc = lax.axis_size("ep"), lax.axis_size("corner")
    endpoints = rows * n
    bins = bin_edges.shape[0]
    combos = 2 * corners
    blocks = rows // LANES
    line = n // PAIR
    chunk = GROUPS // n
    f32 = jnp.float32

    def by_block(v):
        return v.reshape(corners, blocks, LANES).transpose(1, 0, 2).reshape(blocks * corners, LANES)

    vmem = pl.BlockSpec(memory_space=pltpu.VMEM)
    dma = pltpu.SemaphoreType.DMA
    hist, stats, worst = pl.pallas_call(
        functools.partial(report, n, nc, GROUPS * bins / endpoints, make_plan(combos)),
        out_shape=(
            jax.ShapeDtypeStruct((combos, n, chunk, bins), f32),
            jax.ShapeDtypeStruct((3 * combos, LANES), f32),
            jax.ShapeDtypeStruct((2 * blocks, LANES), f32),
        ),
        in_specs=[pl.BlockSpec(memory_space=pltpu.HBM)] * 6,
        out_specs=[vmem] * 3,
        scratch_shapes=[pltpu.VMEM((corners * blocks, LANES), f32)] * 4
        + [
            pltpu.VMEM((blocks, LANES), jnp.int32),
            pltpu.VMEM((bins // LANES, LANES), jnp.int32),
            dma((6,)),
            pltpu.VMEM((FIELDS, blocks, LANES), f32),
            pltpu.VMEM((blocks, LANES), f32),
            pltpu.VMEM((blocks // SPAN, LANES, LANES), f32),
            pltpu.VMEM((SUBS * blocks, LANES), f32),
            pltpu.VMEM((LANES + PACK, 4 * GROUPS), f32),
            pltpu.VMEM((2 * blocks, LANES), f32),
            pltpu.VMEM((nc, 2 * blocks // nc, LANES), f32),
            pltpu.VMEM((combos, LANES), f32),
            pltpu.VMEM((combos, PAIR, line, chunk, bins), f32),
            pltpu.VMEM((combos, n, chunk, bins), f32),
            pltpu.VMEM((3 * combos, LANES), f32),
            pltpu.VMEM((n, 3 * combos, LANES), f32),
        ]
        + [dma((combos, n))] * 6
        + [dma((n,))] * 2
        + [dma((nc,))] * 4,
        compiler_params=pltpu.CompilerParams(
            collective_id=0, has_side_effects=True, vmem_limit_bytes=24 * 1024 * 1024
        ),
        name="report",
    )(
        *[
            pltpu.with_memory_space_constraint(v, pltpu.HBM)
            for v in (
                by_block(required), by_block(arrival), by_block(hold_required),
                by_block(early_arrival), part_ids.reshape(blocks, LANES),
                bin_edges.reshape(bins // LANES, LANES),
            )
        ]
    )
    part_hist, part_tns, part_share, tns, wns, worst = pl.pallas_call(
        functools.partial(finish_kernel, endpoints),
        out_shape=(
            jax.ShapeDtypeStruct((GROUPS, corners, 2, bins), f32),
            jax.ShapeDtypeStruct((corners, 2, GROUPS), f32),
            jax.ShapeDtypeStruct((1, GROUPS), f32),
            jax.ShapeDtypeStruct((corners, 2), f32),
            jax.ShapeDtypeStruct((corners, 2), f32),
            jax.ShapeDtypeStruct((2, rows), f32),
        ),
        in_specs=[vmem] * 3,
        out_specs=[vmem] * 6,
        compiler_params=pltpu.CompilerParams(vmem_limit_bytes=8 * 1024 * 1024),
        name="finish",
    )(hist.reshape(combos, GROUPS, bins), stats, worst)
    return (part_hist, part_tns.transpose(2, 0, 1), part_share[0], tns, wns, worst)


def solution(mesh):
    in_specs = (
        P("corner", "ep"),
        P("corner", "ep"),
        P("corner", "ep"),
        P("corner", "ep"),
        P("ep"),
        P(),
    )
    out_specs = (
        P(None, "corner", None, None),
        P(None, "corner", None),
        P(),
        P("corner", None),
        P("corner", None),
        P(None, "ep"),
    )
    return jax.shard_map(
        on_device, mesh=mesh, in_specs=in_specs, out_specs=out_specs, check_vma=False
    )
```

```python
import functools
import jax
import jax.numpy as jnp
from jax import lax
from jax.experimental import pallas as pl
from jax.experimental.pallas import tpu as pltpu
from jax.sharding import PartitionSpec as P

GROUPS = 64
LANES = 128
SUBS = 8
SPAN = 128
AHEAD = 4
PACK = 16
PAIR = 2
FIELDS = 4
MESH = pl.DeviceIdType.MESH


def pick(table, index):
    return jnp.take_along_axis(table, index, axis=1, mode="promise_in_bounds")


def make_tables(edges_ref):
    nodes = edges_ref[...].astype(jnp.float32) * 0.001
    lane = lax.broadcasted_iota(jnp.int32, (SUBS, LANES), 1)
    rows = [jnp.broadcast_to(nodes[q : q + 1], (SUBS, LANES)) for q in range(4)]

    def gathered(place):
        index = place & (LANES - 1)
        value = pick(rows[3], index)
        for q in (2, 1, 0):
            value = jnp.where(place < LANES * (q + 1), pick(rows[q], index), value)
        return value

    def same(row):
        return pick(row, jnp.zeros((SUBS, LANES), jnp.int32))

    eighths = [same(rows[k // 2]) if k % 2 == 0 else gathered(jnp.full((SUBS, LANES), 64 * k, jnp.int32)) for k in range(8)]
    steps = []
    for size in (16, 4, 1):
        steps.append([gathered((4 * size * lane + size * j) & 511) for j in (1, 2, 3)])
    return eighths, steps


def search(tables, slack):
    eighths, steps = tables
    level = jnp.minimum(jnp.maximum(slack, eighths[0]), 0.0)
    top = level >= eighths[4]
    low = jnp.where(top, eighths[4], eighths[0])
    high = jnp.where(top, 0.0, eighths[4])
    value = jnp.where(top, eighths[6], eighths[2])
    above = level >= value
    low = jnp.where(above, value, low)
    high = jnp.where(above, high, value)
    part = jnp.where(top, 2, 0) + jnp.where(above, 1, 0)
    value = jnp.where(
        top, jnp.where(above, eighths[7], eighths[5]), jnp.where(above, eighths[3], eighths[1])
    )
    above = level >= value
    low = jnp.where(above, value, low)
    high = jnp.where(above, high, value)
    index = part + part
    index = jnp.where(above, index + 1, index)
    for first_at, middle, last_at in steps:
        value = pick(middle, index)
        top = level >= value
        low = jnp.where(top, value, low)
        high = jnp.where(top, high, value)
        value = jnp.where(top, pick(last_at, index), pick(first_at, index))
        above = level >= value
        low = jnp.where(above, value, low)
        high = jnp.where(above, high, value)
        index = 4 * index
        index = jnp.where(top, index + 2, index)
        index = jnp.where(above, index + 1, index)
    scale = 1.0 / (high - low)
    first = (high - level) * scale
    second = (level - low) * scale
    odd_at = (index >> 1) & 63
    even_at = jnp.where(above, odd_at + 1, odd_at)
    even = jnp.where(above, second, first)
    odd = jnp.where(above, first, second)
    return part, even_at, odd_at, even, odd


def report_kernel(
    n, nc, density, plan, accs, spare,
    req_hbm, arr_hbm, hreq_hbm, early_hbm, ids_hbm, edges_hbm,
    hist_out, stats_out, worst_out,
    req, arr, hreq, early, ids, edges, into,
    marks, codes, turned, tail, acc, worst, worst_in, least,
    hist, all_in, stats, stats_in,
    ls, lr, gs, gr, fs, fr, ss, sr, ws, wr, vs, vr,
):
    corners = hist.shape[0] // 2
    combos = 2 * corners
    blocks = ids.shape[0]
    steps = blocks // SUBS
    chunk = GROUPS // n
    line = n // PAIR
    share = worst_out.shape[0] // nc
    narrow = jnp.bfloat16
    f32 = jnp.float32
    me = lax.axis_index("ep")
    mc = lax.axis_index("corner")
    mx = lax.rem(me, PAIR)
    mz = me // PAIR
    other = PAIR - 1 - mx
    mine = mx * line + mz

    loads = []
    for k, (src, dst) in enumerate((
        (edges_hbm, edges), (req_hbm, req), (arr_hbm, arr), (ids_hbm, ids), (early_hbm, early), (hreq_hbm, hreq)
    )):
        loads.append(pltpu.make_async_copy(src, dst, into.at[k]))
        loads[-1].start()

    barrier = pltpu.get_barrier_semaphore()
    for d in range(1, n):
        pl.semaphore_signal(
            barrier, inc=1, device_id={"ep": lax.rem(me + d, n)}, device_id_type=MESH
        )
    for d in range(1, nc):
        pl.semaphore_signal(
            barrier, inc=1, device_id={"corner": lax.rem(mc + d, nc)}, device_id_type=MESH
        )

    def send(src, dst, s_sem, r_sem, target):
        copy = pltpu.make_async_remote_copy(
            src_ref=src, dst_ref=dst, send_sem=s_sem, recv_sem=r_sem,
            device_id=target, device_id_type=MESH,
        )
        copy.start()
        return copy

    def rows_of(k):
        return pl.ds(pl.multiple_of(k * share, SUBS), share)

    row = lax.broadcasted_iota(jnp.int32, (SUBS, LANES), 0)
    fresh = jnp.where(row == 3, 1.0, 0.0).astype(f32)

    def clear(step, carry):
        tail[pl.ds(pl.multiple_of(SUBS * step, SUBS), SUBS), :] = fresh
        return carry

    lax.fori_loop(0, blocks, clear, 0, unroll=8)
    loads[0].wait()
    tables = make_tables(edges)
    sources = ((req, arr), (early, hreq))

    mins = []

    def share_worst():
        def smallest(step, carry):
            for kind, (plus, minus) in enumerate(sources):
                low = None
                for c in range(corners):
                    at = pl.ds(corners * SUBS * step + c, SUBS, stride=corners)
                    slack = plus[at, :] - minus[at, :]
                    low = slack if low is None else jnp.minimum(low, slack)
                worst[pl.ds(2 * SUBS * step + kind, SUBS, stride=2), :] = low
            return carry

        lax.fori_loop(0, steps, smallest, 0, unroll=4)
        pl.semaphore_wait(barrier, n - 1 + nc - 1)
        for d in range(1, nc):
            t = lax.rem(mc + d, nc)
            mins.append(send(worst.at[rows_of(t)], worst_in.at[d], ws.at[d], wr.at[d], {"corner": t}))

    def find(r):
        kind, c = r // corners, r % corners
        plus, minus = sources[kind]

        def body(step, low):
            at = pl.ds(corners * SUBS * step + c, SUBS, stride=corners)
            here = pl.ds(pl.multiple_of(step * SUBS, SUBS), SUBS)
            slack = plus[at, :] - minus[at, :]
            part, even_at, odd_at, even, odd = search(tables, slack)
            codes[here, :] = (part * GROUPS + ids[here, :]).astype(f32)
            marks[0, here, :] = even_at.astype(f32)
            marks[1, here, :] = odd_at.astype(f32)
            marks[2, here, :] = even
            marks[3, here, :] = odd
            negative = jnp.minimum(slack, 0.0)
            coarse = negative.astype(narrow).astype(f32)
            over = jnp.where(even_at == 64, even, 0.0)
            for q, v in enumerate((over, coarse, negative - coarse)):
                tail[pl.ds(SUBS * SUBS * step + q, SUBS, stride=SUBS), :] = v
            return jnp.minimum(low, slack)

        start = jnp.full((SUBS, LANES), jnp.inf, f32)
        low = lax.fori_loop(0, steps, body, start, unroll=16)
        low = jnp.min(jnp.min(low, axis=1, keepdims=True), axis=0, keepdims=True)
        least[r : r + 1] = jnp.broadcast_to(low, (1, LANES))
        for s in range(blocks // SPAN):
            turned[s, :, :SPAN] = codes[s * SPAN : (s + 1) * SPAN].T

    iota = lax.broadcasted_iota(jnp.int32, (PACK, LANES), 0).astype(f32).astype(narrow)
    zero = jnp.zeros((PACK, LANES), narrow)
    width = 4 * GROUPS
    code_iota = lax.broadcasted_iota(jnp.int32, (LANES, width), 1).astype(f32).astype(narrow)
    code_zero = jnp.zeros((LANES, width), narrow)
    code_one = jnp.ones((LANES, width), narrow)

    tiles = SPAN // 2
    whole = blocks // SPAN

    def push(columns, p):
        parts = []
        for t in (2 * p, 2 * p + 1):
            code = jnp.broadcast_to(columns[:, t : t + 1], (LANES, width))
            parts.append(jnp.where(code == code_iota, code_one, code_zero))
        pltpu.matmul_push_rhs(
            jnp.concatenate(parts, axis=0), staging_register=(p // 2) % 2, mxu_index=p % 2
        )

    def left(at):
        def spread(q):
            row = marks[q, pl.ds(at, 1), :]
            return jnp.broadcast_to(row, (PACK, LANES)).astype(narrow)

        even_at, odd_at, even, odd = (spread(q) for q in range(FIELDS))
        parts = []
        for place, v in ((even_at, even), (odd_at, odd)):
            for start in range(0, 64, PACK):
                parts.append(jnp.where(place == iota + narrow(start), v, zero))
        rest = tail[pl.ds(pl.multiple_of(SUBS * at, SUBS), SUBS), :]
        rest = jnp.concatenate([rest, jnp.zeros((SUBS, LANES), f32)], axis=0)
        return jnp.concatenate(parts + [rest.astype(narrow)], axis=0)

    def begin():
        columns = turned[0, :, :SPAN].astype(narrow)
        for p in range(AHEAD):
            push(columns, p)

    def product(first, last):
        def body(s, carry):
            base = pl.multiple_of(s * SPAN, SPAN)
            columns = turned[s, :, :SPAN].astype(narrow)
            later = turned[jnp.minimum(s + 1, whole - 1), :, :SPAN].astype(narrow)
            for p in range(tiles):
                pltpu.matmul_acc_lhs(
                    accs[p % 2],
                    jnp.concatenate([left(base + 2 * p), left(base + 2 * p + 1)], axis=1),
                    load_staged_rhs=(p // 2) % 2,
                )
                if p + AHEAD < tiles:
                    push(columns, p + AHEAD)
                else:
                    push(later, p + AHEAD - tiles)
            return carry

        lax.fori_loop(first, last, body, 0)

    def drain():
        nothing = jnp.zeros((PACK, width), narrow)
        for p in range(AHEAD):
            pltpu.matmul_acc_lhs(spare[p % 2], nothing, load_staged_rhs=(p // 2) % 2)

    lane = lax.broadcasted_iota(jnp.int32, (1, width), 1)

    def fold(v):
        v = v[:, :LANES] + v[:, LANES:]
        return v + pltpu.roll(jnp.broadcast_to(v, (SUBS, LANES)), GROUPS, 1)[0:1]

    def settle(r):
        drain()
        acc[...] = pltpu.matmul_pop(accs[0]) + pltpu.matmul_pop(accs[1])
        full = acc[LANES : LANES + SUBS]
        over = pltpu.roll(jnp.broadcast_to(full[0:1], (SUBS, width)), GROUPS, 1)[0:1]
        acc[0:1] += jnp.where(lane >= GROUPS, over, 0.0)
        turned = acc[0:LANES].T
        for x in range(PAIR):
            for z in range(line):
                for g in range(4):
                    top = g * GROUPS + (x * line + z) * chunk
                    hist[r, x, z, :, g * LANES : (g + 1) * LANES] = turned[top : top + chunk]
        stats[r : r + 1] = fold(full[1:2] + full[2:3])
        if r == 0:
            stats[combos : combos + 1] = fold(full[3:4])

    def pair_of(z):
        return {"ep": z * PAIR + other}

    def line_of(z):
        return {"ep": z * PAIR + mx}

    weave_lane = lax.broadcasted_iota(jnp.int32, (chunk, LANES), 1)
    weave = (weave_lane >> 1) + (weave_lane & 1) * 64

    done = []

    def all_send(r):
        copies = []
        for d in range(1, n):
            t = lax.rem(me + d, n)
            src = hist.at[r, lax.rem(t, PAIR), t // PAIR]
            copies.append(send(src, all_in.at[r, d], ls.at[r, d], lr.at[r, d], {"ep": t}))
        return copies

    def all_sum(r, copies):
        total = hist[r, mx, mz]
        for d in range(1, n):
            copies[d - 1].wait_recv()
            total += all_in[r, d]
        for g in range(total.shape[1] // LANES):
            at = slice(g * LANES, (g + 1) * LANES)
            hist_out[r, mine, :, at] = pick(total[:, at], weave) * density
        done.extend(copies)

    def all_gather(r, copies):
        all_sum(r, copies)
        part = hist_out.at[r, mine]
        back = []
        for d in range(1, n):
            t = lax.rem(me + d, n)
            back.append(send(part, part, gs.at[r, d], gr.at[r, d], {"ep": t}))
        return back

    def line_gather(r, copies):
        all_sum(r, copies)
        part = hist_out.at[r, mine]
        back = []
        for d in range(1, line):
            t = lax.rem(mz + d, line)
            back.append(send(part, part, gs.at[r, d], gr.at[r, d], line_of(t)))
        return back

    def forward(r, back):
        for copy in back:
            copy.wait_recv()
        part = hist_out.at[r, pl.ds(mx * line, line)]
        return back, [send(part, part, fs.at[r], fr.at[r], pair_of(mz))]

    pltpu.matmul_pop(accs[0])
    pltpu.matmul_pop(accs[1])
    pltpu.matmul_pop(spare[0])
    pltpu.matmul_pop(spare[1])
    stats[...] = jnp.zeros_like(stats)

    backs, ended, all_sent = {}, {}, {}
    sent_only = []
    spread_out = []
    half = whole // 2

    def progress(slot):
        for action, r in plan.get(slot, ()):
            if action == "all":
                all_sent[r] = all_send(r)
            elif action == "all_gather":
                ended[r] = all_gather(r, all_sent[r])
            elif action == "line_gather":
                backs[r] = line_gather(r, all_sent[r])
            elif action == "forward":
                got, ends = forward(r, backs[r])
                sent_only.extend(got)
                ended[r] = ends
            elif action == "worst":
                for copy in mins:
                    copy.wait_recv()
                low = worst[rows_of(mc)]
                for d in range(1, nc):
                    low = jnp.minimum(low, worst_in[d])
                worst_out[rows_of(mc)] = low
                for d in range(1, nc):
                    t = lax.rem(mc + d, nc)
                    part = worst_out.at[rows_of(mc)]
                    spread_out.append(send(part, part, vs.at[d], vr.at[d], {"corner": t}))

    for r in range(combos):
        if r == 0:
            for load in loads[1:4]:
                load.wait()
        find(r)
        if r == 0:
            for load in loads[4:]:
                load.wait()
            share_worst()
        begin()
        progress((r, 0))
        product(0, half)
        progress((r, 1))
        product(half, whole)
        settle(r)
        progress((r, 2))

    stats[combos * 2 : combos * 3] = least[0:combos]
    shares = []
    for d in range(1, n):
        t = lax.rem(me + d, n)
        shares.append(send(stats, stats_in.at[me], ss.at[d], sr.at[d], {"ep": t}))
    progress("end")
    for copy in shares:
        copy.wait_recv()
    stats_in[me] = stats[...]
    added = stats_in[0, 0 : 2 * combos]
    lowest = stats_in[0, 2 * combos : 3 * combos]
    for k in range(1, n):
        added += stats_in[k, 0 : 2 * combos]
        lowest = jnp.minimum(lowest, stats_in[k, 2 * combos : 3 * combos])
    stats_out[0 : 2 * combos] = added
    stats_out[2 * combos : 3 * combos] = lowest
    for copy in spread_out:
        copy.wait_recv()
    for r in ended:
        for copy in ended[r]:
            copy.wait_recv()
    for copy in mins + done + sent_only + shares + spread_out:
        copy.wait_send()
    for r in ended:
        for copy in ended[r]:
            copy.wait_send()


def report(n, nc, density, plan, *refs):
    def body(*units):
        report_kernel(n, nc, density, plan, units[:2], units[2:], *refs)

    units = [
        pltpu.ACC(q)((rows, 4 * GROUPS), jnp.float32)
        for rows in (LANES + PACK, PACK)
        for q in range(2)
    ]
    pl.run_scoped(body, *units)


def finish_kernel(endpoints, hist, stats, worst, hist_out, tns_out, share_out, total_out, least_out, worst_out):
    corners = total_out.shape[0]
    combos = 2 * corners
    share = GROUPS / endpoints
    for m in range(2):
        for c in range(corners):
            r = m * corners + c
            hist_out[:, c, m, :] = hist[r]
            row = stats[r : r + 1, :GROUPS]
            tns_out[c, m : m + 1, :] = row * share
            total = jnp.sum(row, axis=1, keepdims=True) * (1.0 / endpoints)
            total_out[c : c + 1, m : m + 1] = total
            least_out[c : c + 1, m : m + 1] = stats[2 * combos + r : 2 * combos + r + 1, 0:1]
    share_out[...] = stats[combos : combos + 1, :GROUPS] * share
    for j in range(worst.shape[0] // 2):
        worst_out[:, j * LANES : (j + 1) * LANES] = worst[2 * j : 2 * j + 2, :]


def make_plan(combos):
    last = combos - 1
    plan = {(1, 0): [("worst", 0)], "end": []}
    for r in range(combos):
        plan[r, 2] = [("all", r)]
        gather = [("line_gather", r)] if r < last else [("all_gather", r)]
        if r < last - 1:
            plan[r + 2, 0] = gather
            if r > 0:
                plan[r + 2, 0].append(("forward", r - 1))
        else:
            if r == last and last > 1:
                plan["end"].append(("forward", last - 2))
            plan["end"] += gather
    plan["end"].append(("forward", last - 1))
    return plan


def on_device(required, arrival, hold_required, early_arrival, part_ids, bin_edges):
    corners, rows = required.shape
    n, nc = lax.axis_size("ep"), lax.axis_size("corner")
    endpoints = rows * n
    bins = bin_edges.shape[0]
    combos = 2 * corners
    blocks = rows // LANES
    line = n // PAIR
    chunk = GROUPS // n
    f32 = jnp.float32

    def by_block(v):
        return v.reshape(corners, blocks, LANES).transpose(1, 0, 2).reshape(blocks * corners, LANES)

    vmem = pl.BlockSpec(memory_space=pltpu.VMEM)
    dma = pltpu.SemaphoreType.DMA
    hist, stats, worst = pl.pallas_call(
        functools.partial(report, n, nc, GROUPS * bins / endpoints, make_plan(combos)),
        out_shape=(
            jax.ShapeDtypeStruct((combos, n, chunk, bins), f32),
            jax.ShapeDtypeStruct((3 * combos, LANES), f32),
            jax.ShapeDtypeStruct((2 * blocks, LANES), f32),
        ),
        in_specs=[pl.BlockSpec(memory_space=pltpu.HBM)] * 6,
        out_specs=[vmem] * 3,
        scratch_shapes=[pltpu.VMEM((corners * blocks, LANES), f32)] * 4
        + [
            pltpu.VMEM((blocks, LANES), jnp.int32),
            pltpu.VMEM((bins // LANES, LANES), jnp.int32),
            dma((6,)),
            pltpu.VMEM((FIELDS, blocks, LANES), f32),
            pltpu.VMEM((blocks, LANES), f32),
            pltpu.VMEM((blocks // SPAN, LANES, LANES), f32),
            pltpu.VMEM((SUBS * blocks, LANES), f32),
            pltpu.VMEM((LANES + PACK, 4 * GROUPS), f32),
            pltpu.VMEM((2 * blocks, LANES), f32),
            pltpu.VMEM((nc, 2 * blocks // nc, LANES), f32),
            pltpu.VMEM((combos, LANES), f32),
            pltpu.VMEM((combos, PAIR, line, chunk, bins), f32),
            pltpu.VMEM((combos, n, chunk, bins), f32),
            pltpu.VMEM((3 * combos, LANES), f32),
            pltpu.VMEM((n, 3 * combos, LANES), f32),
        ]
        + [dma((combos, n))] * 4
        + [dma((combos,))] * 2
        + [dma((n,))] * 2
        + [dma((nc,))] * 4,
        compiler_params=pltpu.CompilerParams(
            collective_id=0, has_side_effects=True, vmem_limit_bytes=24 * 1024 * 1024
        ),
        name="report",
    )(
        *[
            pltpu.with_memory_space_constraint(v, pltpu.HBM)
            for v in (
                by_block(required), by_block(arrival), by_block(hold_required),
                by_block(early_arrival), part_ids.reshape(blocks, LANES),
                bin_edges.reshape(bins // LANES, LANES),
            )
        ]
    )
    part_hist, part_tns, part_share, tns, wns, worst = pl.pallas_call(
        functools.partial(finish_kernel, endpoints),
        out_shape=(
            jax.ShapeDtypeStruct((GROUPS, corners, 2, bins), f32),
            jax.ShapeDtypeStruct((corners, 2, GROUPS), f32),
            jax.ShapeDtypeStruct((1, GROUPS), f32),
            jax.ShapeDtypeStruct((corners, 2), f32),
            jax.ShapeDtypeStruct((corners, 2), f32),
            jax.ShapeDtypeStruct((2, rows), f32),
        ),
        in_specs=[vmem] * 3,
        out_specs=[vmem] * 6,
        compiler_params=pltpu.CompilerParams(vmem_limit_bytes=8 * 1024 * 1024),
        name="finish",
    )(hist.reshape(combos, GROUPS, bins), stats, worst)
    return (part_hist, part_tns.transpose(2, 0, 1), part_share[0], tns, wns, worst)


def solution(mesh):
    in_specs = (
        P("corner", "ep"),
        P("corner", "ep"),
        P("corner", "ep"),
        P("corner", "ep"),
        P("ep"),
        P(),
    )
    out_specs = (
        P(None, "corner", None, None),
        P(None, "corner", None),
        P(),
        P("corner", None),
        P("corner", None),
        P(None, "ep"),
    )
    return jax.shard_map(
        on_device, mesh=mesh, in_specs=in_specs, out_specs=out_specs, check_vma=False
    )
```

```python
import functools
import jax
import jax.numpy as jnp
from jax import lax
from jax.experimental import pallas as pl
from jax.experimental.pallas import tpu as pltpu
from jax.sharding import PartitionSpec as P

GROUPS = 64
LANES = 128
SUBS = 8
SPAN = 128
AHEAD = 4
PACK = 16
PAIR = 2
FIELDS = 4
MESH = pl.DeviceIdType.MESH


def pick(table, index):
    return jnp.take_along_axis(table, index, axis=1, mode="promise_in_bounds")


def make_tables(edges_ref):
    nodes = edges_ref[...].astype(jnp.float32) * 0.001
    lane = lax.broadcasted_iota(jnp.int32, (SUBS, LANES), 1)
    rows = [jnp.broadcast_to(nodes[q : q + 1], (SUBS, LANES)) for q in range(4)]

    def gathered(place):
        index = place & (LANES - 1)
        value = pick(rows[3], index)
        for q in (2, 1, 0):
            value = jnp.where(place < LANES * (q + 1), pick(rows[q], index), value)
        return value

    def same(row):
        return pick(row, jnp.zeros((SUBS, LANES), jnp.int32))

    eighths = [same(rows[k // 2]) if k % 2 == 0 else gathered(jnp.full((SUBS, LANES), 64 * k, jnp.int32)) for k in range(8)]
    steps = []
    for size in (16, 4, 1):
        steps.append([gathered((4 * size * lane + size * j) & 511) for j in (1, 2, 3)])
    return eighths, steps


def search(tables, slack):
    eighths, steps = tables
    level = jnp.minimum(jnp.maximum(slack, eighths[0]), 0.0)
    top = level >= eighths[4]
    low = jnp.where(top, eighths[4], eighths[0])
    high = jnp.where(top, 0.0, eighths[4])
    value = jnp.where(top, eighths[6], eighths[2])
    above = level >= value
    low = jnp.where(above, value, low)
    high = jnp.where(above, high, value)
    part = jnp.where(top, 2, 0) + jnp.where(above, 1, 0)
    value = jnp.where(
        top, jnp.where(above, eighths[7], eighths[5]), jnp.where(above, eighths[3], eighths[1])
    )
    above = level >= value
    low = jnp.where(above, value, low)
    high = jnp.where(above, high, value)
    index = part + part
    index = jnp.where(above, index + 1, index)
    for first_at, middle, last_at in steps:
        value = pick(middle, index)
        top = level >= value
        low = jnp.where(top, value, low)
        high = jnp.where(top, high, value)
        value = jnp.where(top, pick(last_at, index), pick(first_at, index))
        above = level >= value
        low = jnp.where(above, value, low)
        high = jnp.where(above, high, value)
        index = 4 * index
        index = jnp.where(top, index + 2, index)
        index = jnp.where(above, index + 1, index)
    scale = 1.0 / (high - low)
    first = (high - level) * scale
    second = (level - low) * scale
    odd_at = (index >> 1) & 63
    even_at = jnp.where(above, odd_at + 1, odd_at)
    even = jnp.where(above, second, first)
    odd = jnp.where(above, first, second)
    return part, even_at, odd_at, even, odd


def report_kernel(
    n, nc, density, plan, accs, spare,
    req_hbm, arr_hbm, hreq_hbm, early_hbm, ids_hbm, edges_hbm,
    hist_out, stats_out, worst_out,
    req, arr, hreq, early, ids, edges, into,
    marks, codes, turned, tail, acc, worst, worst_in, least,
    hist, all_in, stats, stats_in,
    ls, lr, gs, gr, fs, fr, ss, sr, ws, wr, vs, vr,
):
    corners = hist.shape[0] // 2
    combos = 2 * corners
    blocks = ids.shape[0]
    steps = blocks // SUBS
    chunk = GROUPS // n
    line = n // PAIR
    share = worst_out.shape[0] // nc
    narrow = jnp.bfloat16
    f32 = jnp.float32
    me = lax.axis_index("ep")
    mc = lax.axis_index("corner")
    mx = lax.rem(me, PAIR)
    mz = me // PAIR
    other = PAIR - 1 - mx
    mine = mx * line + mz

    loads = []
    for k, (src, dst) in enumerate((
        (edges_hbm, edges), (req_hbm, req), (arr_hbm, arr), (ids_hbm, ids), (early_hbm, early), (hreq_hbm, hreq)
    )):
        loads.append(pltpu.make_async_copy(src, dst, into.at[k]))
        loads[-1].start()

    barrier = pltpu.get_barrier_semaphore()
    for d in range(1, n):
        pl.semaphore_signal(
            barrier, inc=1, device_id={"ep": lax.rem(me + d, n)}, device_id_type=MESH
        )
    for d in range(1, nc):
        pl.semaphore_signal(
            barrier, inc=1, device_id={"corner": lax.rem(mc + d, nc)}, device_id_type=MESH
        )

    def send(src, dst, s_sem, r_sem, target):
        copy = pltpu.make_async_remote_copy(
            src_ref=src, dst_ref=dst, send_sem=s_sem, recv_sem=r_sem,
            device_id=target, device_id_type=MESH,
        )
        copy.start()
        return copy

    def rows_of(k):
        return pl.ds(pl.multiple_of(k * share, SUBS), share)

    row = lax.broadcasted_iota(jnp.int32, (SUBS, LANES), 0)
    fresh = jnp.where(row == 3, 1.0, 0.0).astype(f32)

    def clear(step, carry):
        tail[pl.ds(pl.multiple_of(SUBS * step, SUBS), SUBS), :] = fresh
        return carry

    lax.fori_loop(0, blocks, clear, 0, unroll=8)
    loads[0].wait()
    tables = make_tables(edges)
    sources = ((req, arr), (early, hreq))

    mins = []

    def share_worst():
        def smallest(step, carry):
            for kind, (plus, minus) in enumerate(sources):
                low = None
                for c in range(corners):
                    at = pl.ds(corners * SUBS * step + c, SUBS, stride=corners)
                    slack = plus[at, :] - minus[at, :]
                    low = slack if low is None else jnp.minimum(low, slack)
                worst[pl.ds(2 * SUBS * step + kind, SUBS, stride=2), :] = low
            return carry

        lax.fori_loop(0, steps, smallest, 0, unroll=4)
        pl.semaphore_wait(barrier, n - 1 + nc - 1)
        for d in range(1, nc):
            t = lax.rem(mc + d, nc)
            mins.append(send(worst.at[rows_of(t)], worst_in.at[d], ws.at[d], wr.at[d], {"corner": t}))

    def find(r):
        kind, c = r // corners, r % corners
        plus, minus = sources[kind]

        def body(step, low):
            at = pl.ds(corners * SUBS * step + c, SUBS, stride=corners)
            here = pl.ds(pl.multiple_of(step * SUBS, SUBS), SUBS)
            slack = plus[at, :] - minus[at, :]
            part, even_at, odd_at, even, odd = search(tables, slack)
            codes[here, :] = (part * GROUPS + ids[here, :]).astype(f32)
            marks[0, here, :] = even_at.astype(f32)
            marks[1, here, :] = odd_at.astype(f32)
            marks[2, here, :] = even
            marks[3, here, :] = odd
            negative = jnp.minimum(slack, 0.0)
            coarse = negative.astype(narrow).astype(f32)
            over = jnp.where(even_at == 64, even, 0.0)
            for q, v in enumerate((over, coarse, negative - coarse)):
                tail[pl.ds(SUBS * SUBS * step + q, SUBS, stride=SUBS), :] = v
            return jnp.minimum(low, slack)

        start = jnp.full((SUBS, LANES), jnp.inf, f32)
        low = lax.fori_loop(0, steps, body, start, unroll=16)
        low = jnp.min(jnp.min(low, axis=1, keepdims=True), axis=0, keepdims=True)
        least[r : r + 1] = jnp.broadcast_to(low, (1, LANES))
        for s in range(blocks // SPAN):
            turned[s, :, :SPAN] = codes[s * SPAN : (s + 1) * SPAN].T

    iota = lax.broadcasted_iota(jnp.int32, (PACK, LANES), 0).astype(f32).astype(narrow)
    zero = jnp.zeros((PACK, LANES), narrow)
    width = 4 * GROUPS
    code_iota = lax.broadcasted_iota(jnp.int32, (LANES, width), 1).astype(f32).astype(narrow)
    code_zero = jnp.zeros((LANES, width), narrow)
    code_one = jnp.ones((LANES, width), narrow)

    tiles = SPAN // 2
    whole = blocks // SPAN

    def push(columns, p):
        parts = []
        for t in (2 * p, 2 * p + 1):
            code = jnp.broadcast_to(columns[:, t : t + 1], (LANES, width))
            parts.append(jnp.where(code == code_iota, code_one, code_zero))
        pltpu.matmul_push_rhs(
            jnp.concatenate(parts, axis=0), staging_register=(p // 2) % 2, mxu_index=p % 2
        )

    def left(at):
        def spread(q):
            row = marks[q, pl.ds(at, 1), :]
            return jnp.broadcast_to(row, (PACK, LANES)).astype(narrow)

        even_at, odd_at, even, odd = (spread(q) for q in range(FIELDS))
        parts = []
        for place, v in ((even_at, even), (odd_at, odd)):
            for start in range(0, 64, PACK):
                parts.append(jnp.where(place == iota + narrow(start), v, zero))
        rest = tail[pl.ds(pl.multiple_of(SUBS * at, SUBS), SUBS), :]
        rest = jnp.concatenate([rest, jnp.zeros((SUBS, LANES), f32)], axis=0)
        return jnp.concatenate(parts + [rest.astype(narrow)], axis=0)

    def begin():
        columns = turned[0, :, :SPAN].astype(narrow)
        for p in range(AHEAD):
            push(columns, p)

    def product(first, last):
        def body(s, carry):
            base = pl.multiple_of(s * SPAN, SPAN)
            columns = turned[s, :, :SPAN].astype(narrow)
            later = turned[jnp.minimum(s + 1, whole - 1), :, :SPAN].astype(narrow)
            for p in range(tiles):
                pltpu.matmul_acc_lhs(
                    accs[p % 2],
                    jnp.concatenate([left(base + 2 * p), left(base + 2 * p + 1)], axis=1),
                    load_staged_rhs=(p // 2) % 2,
                )
                if p + AHEAD < tiles:
                    push(columns, p + AHEAD)
                else:
                    push(later, p + AHEAD - tiles)
            return carry

        lax.fori_loop(first, last, body, 0)

    def drain():
        nothing = jnp.zeros((PACK, width), narrow)
        for p in range(AHEAD):
            pltpu.matmul_acc_lhs(spare[p % 2], nothing, load_staged_rhs=(p // 2) % 2)

    lane = lax.broadcasted_iota(jnp.int32, (1, width), 1)

    def fold(v):
        v = v[:, :LANES] + v[:, LANES:]
        return v + pltpu.roll(jnp.broadcast_to(v, (SUBS, LANES)), GROUPS, 1)[0:1]

    def settle(r):
        drain()
        acc[...] = pltpu.matmul_pop(accs[0]) + pltpu.matmul_pop(accs[1])
        full = acc[LANES : LANES + SUBS]
        over = pltpu.roll(jnp.broadcast_to(full[0:1], (SUBS, width)), GROUPS, 1)[0:1]
        acc[0:1] += jnp.where(lane >= GROUPS, over, 0.0)
        turned = acc[0:LANES].T
        for x in range(PAIR):
            for z in range(line):
                for g in range(4):
                    top = g * GROUPS + (x * line + z) * chunk
                    hist[r, x, z, :, g * LANES : (g + 1) * LANES] = turned[top : top + chunk]
        stats[r : r + 1] = fold(full[1:2] + full[2:3])
        if r == 0:
            stats[combos : combos + 1] = fold(full[3:4])

    def pair_of(z):
        return {"ep": z * PAIR + other}

    def line_of(z):
        return {"ep": z * PAIR + mx}

    weave_lane = lax.broadcasted_iota(jnp.int32, (chunk, LANES), 1)
    weave = (weave_lane >> 1) + (weave_lane & 1) * 64

    done = []

    def all_send(r):
        copies = []
        for d in range(1, n):
            t = lax.rem(me + d, n)
            src = hist.at[r, lax.rem(t, PAIR), t // PAIR]
            copies.append(send(src, all_in.at[r, d], ls.at[r, d], lr.at[r, d], {"ep": t}))
        return copies

    def all_sum(r, copies):
        total = hist[r, mx, mz]
        for d in range(1, n):
            copies[d - 1].wait_recv()
            total += all_in[r, d]
        for g in range(total.shape[1] // LANES):
            at = slice(g * LANES, (g + 1) * LANES)
            hist_out[r, mine, :, at] = pick(total[:, at], weave) * density
        done.extend(copies)

    def all_gather(r, copies):
        all_sum(r, copies)
        part = hist_out.at[r, mine]
        back = []
        for d in range(1, n):
            t = lax.rem(me + d, n)
            back.append(send(part, part, gs.at[r, d], gr.at[r, d], {"ep": t}))
        return back

    def line_gather(r, copies):
        all_sum(r, copies)
        part = hist_out.at[r, mine]
        back = []
        for d in range(1, line):
            t = lax.rem(mz + d, line)
            back.append(send(part, part, gs.at[r, d], gr.at[r, d], line_of(t)))
        return back

    def forward(r, back):
        for copy in back:
            copy.wait_recv()
        part = hist_out.at[r, pl.ds(mx * line, line)]
        return back, [send(part, part, fs.at[r], fr.at[r], pair_of(mz))]

    pltpu.matmul_pop(accs[0])
    pltpu.matmul_pop(accs[1])
    pltpu.matmul_pop(spare[0])
    pltpu.matmul_pop(spare[1])
    stats[...] = jnp.zeros_like(stats)

    backs, ended, all_sent = {}, {}, {}
    sent_only = []
    spread_out = []
    half = whole // 2

    def progress(slot):
        for action, r in plan.get(slot, ()):
            if action == "all":
                all_sent[r] = all_send(r)
            elif action == "all_gather":
                ended[r] = all_gather(r, all_sent[r])
            elif action == "line_gather":
                backs[r] = line_gather(r, all_sent[r])
            elif action == "forward":
                got, ends = forward(r, backs[r])
                sent_only.extend(got)
                ended[r] = ends
            elif action == "worst":
                for copy in mins:
                    copy.wait_recv()
                low = worst[rows_of(mc)]
                for d in range(1, nc):
                    low = jnp.minimum(low, worst_in[d])
                worst_out[rows_of(mc)] = low
                for d in range(1, nc):
                    t = lax.rem(mc + d, nc)
                    part = worst_out.at[rows_of(mc)]
                    spread_out.append(send(part, part, vs.at[d], vr.at[d], {"corner": t}))

    for r in range(combos):
        if r == 0:
            for load in loads[1:4]:
                load.wait()
        find(r)
        if r == 0:
            for load in loads[4:]:
                load.wait()
            share_worst()
        begin()
        progress((r, 0))
        product(0, half)
        progress((r, 1))
        product(half, whole)
        settle(r)
        progress((r, 2))

    stats[combos * 2 : combos * 3] = least[0:combos]
    shares = []
    for d in range(1, n):
        t = lax.rem(me + d, n)
        shares.append(send(stats, stats_in.at[me], ss.at[d], sr.at[d], {"ep": t}))
    progress("end")
    for copy in shares:
        copy.wait_recv()
    stats_in[me] = stats[...]
    added = stats_in[0, 0 : 2 * combos]
    lowest = stats_in[0, 2 * combos : 3 * combos]
    for k in range(1, n):
        added += stats_in[k, 0 : 2 * combos]
        lowest = jnp.minimum(lowest, stats_in[k, 2 * combos : 3 * combos])
    stats_out[0 : 2 * combos] = added
    stats_out[2 * combos : 3 * combos] = lowest
    for copy in spread_out:
        copy.wait_recv()
    for r in ended:
        for copy in ended[r]:
            copy.wait_recv()
    for copy in mins + done + sent_only + shares + spread_out:
        copy.wait_send()
    for r in ended:
        for copy in ended[r]:
            copy.wait_send()


def report(n, nc, density, plan, *refs):
    def body(*units):
        report_kernel(n, nc, density, plan, units[:2], units[2:], *refs)

    units = [
        pltpu.ACC(q)((rows, 4 * GROUPS), jnp.float32)
        for rows in (LANES + PACK, PACK)
        for q in range(2)
    ]
    pl.run_scoped(body, *units)


def finish_kernel(endpoints, hist, stats, worst, hist_out, tns_out, share_out, total_out, least_out, worst_out):
    corners = total_out.shape[0]
    combos = 2 * corners
    share = GROUPS / endpoints
    for m in range(2):
        for c in range(corners):
            r = m * corners + c
            hist_out[:, c, m, :] = hist[r]
            row = stats[r : r + 1, :GROUPS]
            tns_out[c, m : m + 1, :] = row * share
            total = jnp.sum(row, axis=1, keepdims=True) * (1.0 / endpoints)
            total_out[c : c + 1, m : m + 1] = total
            least_out[c : c + 1, m : m + 1] = stats[2 * combos + r : 2 * combos + r + 1, 0:1]
    share_out[...] = stats[combos : combos + 1, :GROUPS] * share
    for j in range(worst.shape[0] // 2):
        worst_out[:, j * LANES : (j + 1) * LANES] = worst[2 * j : 2 * j + 2, :]


def make_plan(combos):
    last = combos - 1
    plan = {(1, 0): [("worst", 0)], "end": []}
    for r in range(combos):
        plan[r, 2] = [("all", r)]
        gather = [("line_gather", r)] if r < last else [("all_gather", r)]
        if r < last - 1:
            plan[r + 2, 1] = gather
            if r > 0:
                plan[r + 2, 1].append(("forward", r - 1))
        else:
            if r == last and last > 1:
                plan["end"].append(("forward", last - 2))
            plan["end"] += gather
    plan["end"].append(("forward", last - 1))
    return plan


def on_device(required, arrival, hold_required, early_arrival, part_ids, bin_edges):
    corners, rows = required.shape
    n, nc = lax.axis_size("ep"), lax.axis_size("corner")
    endpoints = rows * n
    bins = bin_edges.shape[0]
    combos = 2 * corners
    blocks = rows // LANES
    line = n // PAIR
    chunk = GROUPS // n
    f32 = jnp.float32

    def by_block(v):
        return v.reshape(corners, blocks, LANES).transpose(1, 0, 2).reshape(blocks * corners, LANES)

    vmem = pl.BlockSpec(memory_space=pltpu.VMEM)
    dma = pltpu.SemaphoreType.DMA
    hist, stats, worst = pl.pallas_call(
        functools.partial(report, n, nc, GROUPS * bins / endpoints, make_plan(combos)),
        out_shape=(
            jax.ShapeDtypeStruct((combos, n, chunk, bins), f32),
            jax.ShapeDtypeStruct((3 * combos, LANES), f32),
            jax.ShapeDtypeStruct((2 * blocks, LANES), f32),
        ),
        in_specs=[pl.BlockSpec(memory_space=pltpu.HBM)] * 6,
        out_specs=[vmem] * 3,
        scratch_shapes=[pltpu.VMEM((corners * blocks, LANES), f32)] * 4
        + [
            pltpu.VMEM((blocks, LANES), jnp.int32),
            pltpu.VMEM((bins // LANES, LANES), jnp.int32),
            dma((6,)),
            pltpu.VMEM((FIELDS, blocks, LANES), f32),
            pltpu.VMEM((blocks, LANES), f32),
            pltpu.VMEM((blocks // SPAN, LANES, LANES), f32),
            pltpu.VMEM((SUBS * blocks, LANES), f32),
            pltpu.VMEM((LANES + PACK, 4 * GROUPS), f32),
            pltpu.VMEM((2 * blocks, LANES), f32),
            pltpu.VMEM((nc, 2 * blocks // nc, LANES), f32),
            pltpu.VMEM((combos, LANES), f32),
            pltpu.VMEM((combos, PAIR, line, chunk, bins), f32),
            pltpu.VMEM((combos, n, chunk, bins), f32),
            pltpu.VMEM((3 * combos, LANES), f32),
            pltpu.VMEM((n, 3 * combos, LANES), f32),
        ]
        + [dma((combos, n))] * 4
        + [dma((combos,))] * 2
        + [dma((n,))] * 2
        + [dma((nc,))] * 4,
        compiler_params=pltpu.CompilerParams(
            collective_id=0, has_side_effects=True, vmem_limit_bytes=24 * 1024 * 1024
        ),
        name="report",
    )(
        *[
            pltpu.with_memory_space_constraint(v, pltpu.HBM)
            for v in (
                by_block(required), by_block(arrival), by_block(hold_required),
                by_block(early_arrival), part_ids.reshape(blocks, LANES),
                bin_edges.reshape(bins // LANES, LANES),
            )
        ]
    )
    part_hist, part_tns, part_share, tns, wns, worst = pl.pallas_call(
        functools.partial(finish_kernel, endpoints),
        out_shape=(
            jax.ShapeDtypeStruct((GROUPS, corners, 2, bins), f32),
            jax.ShapeDtypeStruct((corners, 2, GROUPS), f32),
            jax.ShapeDtypeStruct((1, GROUPS), f32),
            jax.ShapeDtypeStruct((corners, 2), f32),
            jax.ShapeDtypeStruct((corners, 2), f32),
            jax.ShapeDtypeStruct((2, rows), f32),
        ),
        in_specs=[vmem] * 3,
        out_specs=[vmem] * 6,
        compiler_params=pltpu.CompilerParams(vmem_limit_bytes=8 * 1024 * 1024),
        name="finish",
    )(hist.reshape(combos, GROUPS, bins), stats, worst)
    return (part_hist, part_tns.transpose(2, 0, 1), part_share[0], tns, wns, worst)


def solution(mesh):
    in_specs = (
        P("corner", "ep"),
        P("corner", "ep"),
        P("corner", "ep"),
        P("corner", "ep"),
        P("ep"),
        P(),
    )
    out_specs = (
        P(None, "corner", None, None),
        P(None, "corner", None),
        P(),
        P("corner", None),
        P("corner", None),
        P(None, "ep"),
    )
    return jax.shard_map(
        on_device, mesh=mesh, in_specs=in_specs, out_specs=out_specs, check_vma=False
    )
```
